32 devices in a mesh: batch: 1 (over z), cols: 4 (over y), rows: 8 (over x, core).
Axes of the slice: x: 4, y: 4, z: 1, core: 2. Of those that a mesh axis runs over, the one named last changes fastest.
The devices are a block of a 4x4x8 slice.
Arguments:
- frames: bfloat16 [24, 1, 384, 384, 16], P(None, 'batch', 'rows', 'cols')
- h_init: float32 [1, 384, 384, 64], P('batch', 'rows', 'cols')
- w_x: bfloat16 [3, 3, 16, 192], replicated
- w_hzr: bfloat16 [3, 3, 64, 128], replicated
- w_hn: bfloat16 [3, 3, 64, 64], replicated
- gate_bias: float32 [192], replicated
Outputs:
- output 1: bfloat16 [24, 1, 384, 384, 64], P(None, 'batch', 'rows', 'cols')
- output 2: float32 [1, 384, 384, 64], P('batch', 'rows', 'cols')
All inputs are finite; a program needn't handle non-finite values.
Results may differ from the reference program's by a relative error of at most 0.00441273.
Values are sent between devices in bfloat16 or wider.
A program may use at most 768 MiB of HBM per device.

```python
import jax
import jax.numpy as jnp
from jax import lax

STEPS = 24
BATCH = 1
HEIGHT = 384
WIDTH = 384
CIN = 16
CH = 64


def setup_inputs(seed: int = 0, part: int = 0) -> dict:
    keys = jax.random.split(jax.random.key(seed), 6)
    key_frames = jax.random.fold_in(keys[0], part)
    key_state = jax.random.fold_in(keys[1], part)
    frames = jax.random.normal(key_frames, (STEPS, BATCH, HEIGHT, WIDTH, CIN), jnp.float32).astype(jnp.bfloat16)
    h_init = 0.8 * jax.random.normal(key_state, (BATCH, HEIGHT, WIDTH, CH), jnp.float32)
    w_x = (jax.random.normal(keys[2], (3, 3, CIN, 3 * CH), jnp.float32) * (9 * CIN) ** -0.5).astype(jnp.bfloat16)
    w_hzr = (jax.random.normal(keys[3], (3, 3, CH, 2 * CH), jnp.float32) * (1.5 * (9 * CH) ** -0.5)).astype(jnp.bfloat16)
    w_hn = (jax.random.normal(keys[4], (3, 3, CH, CH), jnp.float32) * (2.0 * (9 * CH) ** -0.5)).astype(jnp.bfloat16)
    gate_bias = 0.5 * jax.random.normal(keys[5], (3 * CH,), jnp.float32)
    return {'frames': frames, 'h_init': h_init, 'w_x': w_x, 'w_hzr': w_hzr, 'w_hn': w_hn, 'gate_bias': gate_bias}


def conv_same(inputs, weights):
    return lax.conv_general_dilated(inputs.astype(jnp.float32), weights.astype(jnp.float32), (1, 1), 'SAME', dimension_numbers=('NHWC', 'HWIO', 'NHWC'), precision=lax.Precision.HIGHEST)


def reference(frames, h_init, w_x, w_hzr, w_hn, gate_bias):
    def one_step(h_prev, frame_t):
        gate_x = conv_same(frame_t, w_x) + gate_bias
        zr_gates = jax.nn.sigmoid(gate_x[..., :2 * CH] + conv_same(h_prev.astype(jnp.bfloat16), w_hzr))
        update = zr_gates[..., :CH]
        reset_hid = (zr_gates[..., CH:] * h_prev).astype(jnp.bfloat16)
        candidate = jnp.tanh(gate_x[..., 2 * CH:] + conv_same(reset_hid, w_hn))
        h_next = (1.0 - update) * candidate + update * h_prev
        return h_next, h_next.astype(jnp.bfloat16)
    h_last, h_seq = lax.scan(one_step, h_init, frames)
    return h_seq, h_last
```

```python
import functools

import jax
import jax.numpy as jnp
from jax import lax
from jax.experimental import pallas as pl
from jax.experimental.pallas import tpu as pltpu
from jax.sharding import PartitionSpec as P

MESH = pl.DeviceIdType.MESH
LANES = 128
BF = jnp.bfloat16
F32 = jnp.float32

ROW_STEPS = 2
HR = 2 * ROW_STEPS
HC = 16
COL_STEPS = HC // 2
ZR_TILES = 9
N_GROUPS = (13, 12)


def store3(buf, base, size, val):
    buf[pl.ds(base, size), :] = pltpu.roll(val, 1, 1)
    buf[pl.ds(base + size, size), :] = val
    buf[pl.ds(base + 2 * size, size), :] = pltpu.roll(val, LANES - 1, 1)


def kernel(n_rows, n_cols, fp, h0, wzr, wn, out, hlast,
           H, HB, RB, XB, Z, XS, OS, CS, CR, RR,
           xs_sem, os_sem, cs_send, cs_recv, rr_send, rr_recv):
    steps, tile_h, ch, tile_w = out.shape
    cin = fp.shape[2]
    total_rows = tile_h + 2 * HR
    row = lax.axis_index('rows')
    col = lax.axis_index('cols')
    has_up, has_down = row > 0, row < n_rows - 1
    has_left, has_right = col > 0, col < n_cols - 1

    for s in range(2):
        for side in range(2):
            CR[s, side] = jnp.zeros(CR.shape[2:], F32)
            RR[s, side] = jnp.zeros(RR.shape[2:], F32)
    barrier = pltpu.get_barrier_semaphore()
    sides = ((has_up, {'rows': row - 1}), (has_down, {'rows': row + 1}),
             (has_left, {'cols': col - 1}), (has_right, {'cols': col + 1}))
    for cond, dev in sides:
        @pl.when(cond)
        def _(dev=dev):
            pl.semaphore_signal(barrier, inc=1, device_id=dev, device_id_type=MESH)
    count = sum(jnp.where(cond, 1, 0) for cond, _ in sides)

    lane = lax.broadcasted_iota(jnp.int32, (ch, LANES), 1)
    slot_of = lane // HC
    ones = jnp.where(lax.broadcasted_iota(jnp.int32, (64, LANES), 0) < 3, 1.0, 0.0).astype(BF)
    left_ok = jnp.where(has_left, 1, 0)
    right_ok = jnp.where(has_right, 1, 0)
    up_ok = jnp.where(has_up, 1, 0)
    down_ok = jnp.where(has_down, 1, 0)
    lane_ok = jnp.where(lane < tile_w, 1, jnp.where(lane < tile_w + HC, right_ok, left_ok))

    def frame_copy(step, slot):
        return pltpu.make_async_copy(fp.at[step], XS.at[slot], xs_sem.at[slot])

    def out_copy(step, slot):
        return pltpu.make_async_copy(OS.at[slot, pl.ds(ROW_STEPS, tile_h)], out.at[step], os_sem.at[slot])

    frame_copy(0, 0).start()

    def init_row(i, _):
        H[i] = jnp.zeros((ch, LANES), F32)
        H[i, :, 0:tile_w] = h0[i - HR]
        return 0
    lax.fori_loop(HR, HR + tile_h, init_row, 0)
    pl.semaphore_wait(barrier, count)

    n_slots = tile_w // HC
    per = LANES // HC

    def col_copies(slot):
        to_left = pltpu.make_async_remote_copy(CS.at[0], CR.at[slot, 1], cs_send.at[0], cs_recv.at[slot, 1], device_id={'cols': col - 1}, device_id_type=MESH)
        to_right = pltpu.make_async_remote_copy(CS.at[1], CR.at[slot, 0], cs_send.at[1], cs_recv.at[slot, 0], device_id={'cols': col + 1}, device_id_type=MESH)
        return to_left, to_right

    def col_exchange(slot):
        def pack(g, _):
            left = jnp.zeros((ch, LANES), F32)
            right = jnp.zeros((ch, LANES), F32)
            for q in range(per):
                val = H[HR + g * per + q]
                moved = pltpu.roll(val, HC * q, 1) if q else val
                left = jnp.where(slot_of == q, moved, left)
                right = jnp.where(slot_of == (n_slots - 1 + q) % per, moved, right)
            CS[0, g] = left
            CS[1, g] = right
            return 0
        lax.fori_loop(0, tile_h // per, pack, 0)
        to_left, to_right = col_copies(slot)

        @pl.when(has_left)
        def _():
            to_left.start()

        @pl.when(has_right)
        def _():
            to_right.start()

        @pl.when(has_left)
        def _():
            to_left.wait_send()
            to_right.wait_recv()

        @pl.when(has_right)
        def _():
            to_right.wait_send()
            to_left.wait_recv()

        def unpack(g, _):
            from_right = CR[slot, 1, g]
            from_left = CR[slot, 0, g]
            for q in range(per):
                i = HR + g * per + q
                s_right = HC * ((n_slots - q) % per)
                s_left = HC * ((per - n_slots - q) % per)
                right = pltpu.roll(from_right, s_right, 1) if s_right else from_right
                left = pltpu.roll(from_left, s_left, 1) if s_left else from_left
                val = jnp.where(lane < tile_w, H[i], jnp.where(lane < tile_w + HC, right, left))
                H[i] = val
                store3(HB, pl.multiple_of(i * (3 * ch), 3 * ch), ch, val.astype(BF))
            return 0
        lax.fori_loop(0, tile_h // per, unpack, 0)

    def row_copies(slot):
        to_up = pltpu.make_async_remote_copy(H.at[pl.ds(HR, HR)], RR.at[slot, 1], rr_send.at[0], rr_recv.at[slot, 1], device_id={'rows': row - 1}, device_id_type=MESH)
        to_down = pltpu.make_async_remote_copy(H.at[pl.ds(tile_h, HR)], RR.at[slot, 0], rr_send.at[1], rr_recv.at[slot, 0], device_id={'rows': row + 1}, device_id_type=MESH)
        return to_up, to_down

    def row_exchange(slot):
        to_up, to_down = row_copies(slot)

        @pl.when(has_up)
        def _():
            to_up.start()

        @pl.when(has_down)
        def _():
            to_down.start()

        @pl.when(has_up)
        def _():
            to_up.wait_send()
            to_down.wait_recv()

        @pl.when(has_down)
        def _():
            to_down.wait_send()
            to_up.wait_recv()

        for i in range(HR):
            for side, at in ((0, i), (1, HR + tile_h + i)):
                val = RR[slot, side, i]
                H[at] = val
                store3(HB, at * 3 * ch, ch, val.astype(BF))

    def zr_tile(i):
        cols = []
        for d in range(2):
            hb = HB[pl.ds(pl.multiple_of((i + d - 1) * (3 * ch), 3 * ch), 9 * ch), :]
            xb = XB[pl.ds(pl.multiple_of((i + d - 1) * (3 * cin), 3 * cin), 9 * cin), :]
            cols.append(jnp.concatenate([hb, xb, ones[:48]], axis=0))
        acc = jnp.dot(wzr[...], jnp.concatenate(cols, axis=1), preferred_element_type=F32)
        gates = jnp.tanh(acc)
        for d in range(2):
            Z[i + d] = gates[:ch, d * LANES:(d + 1) * LANES]
            reset = 0.5 * gates[ch:, d * LANES:(d + 1) * LANES] + 0.5
            store3(RB, pl.multiple_of((i + d) * (3 * ch), 3 * ch), ch, (reset * H[i + d]).astype(BF))

    def n_group(i, slot):
        cols = []
        for p in range(2):
            y = i + 2 * p - 1
            hb = RB[pl.ds(pl.multiple_of(y * (3 * ch), 3 * ch), 12 * ch), :]
            xb = XB[pl.ds(pl.multiple_of(y * (3 * cin), 3 * cin), 12 * cin), :]
            cols.append(jnp.concatenate([hb, xb, ones], axis=0))
        acc = jnp.dot(wn[...], jnp.concatenate(cols, axis=1), preferred_element_type=F32)
        cand = jnp.tanh(acc)
        for p in range(2):
            for dy in range(2):
                at = i + 2 * p + dy
                cand_row = cand[dy * ch:(dy + 1) * ch, p * LANES:(p + 1) * LANES]
                update = 0.5 * Z[at] + 0.5
                row_ok = jnp.where(at < HR, up_ok, jnp.where(at < HR + tile_h, 1, down_ok))
                new = cand_row + update * (H[at] - cand_row)
                new = jnp.where(lane_ok * row_ok != 0, new, 0.0)
                H[at] = new
                new_bf = new.astype(BF)
                store3(HB, pl.multiple_of(at * (3 * ch), 3 * ch), ch, new_bf)
                OS[slot, at - HR + ROW_STEPS] = new_bf[:, :tile_w]

    def one_step(t, j):
        slot = lax.rem(t, 2)
        frame_copy(t, slot).wait()

        def spread(i, _):
            for u in range(8):
                store3(XB, pl.multiple_of((i * 8 + u) * (3 * cin), 3 * cin), cin, XS[slot, i * 8 + u])
            return 0
        lax.fori_loop(0, total_rows // 8, spread, 0)

        @pl.when(t + 1 < steps)
        def _():
            frame_copy(t + 1, 1 - slot).start()

        first = 2 * j + 1
        tiles = (total_rows - 2 * first) // 2
        trip = ZR_TILES
        trips = -(-tiles // trip)
        start = first if first + trips * trip * 2 + 1 <= total_rows else first - 2

        def zr_trip(k, _):
            for u in range(trip):
                zr_tile(start + 2 * (k * trip + u))
            return 0
        lax.fori_loop(0, trips, zr_trip, 0)

        @pl.when(t >= 2)
        def _():
            out_copy(t - 2, slot).wait()

        first = 2 * j + 2
        groups = (total_rows - 2 * first) // 4
        trip = N_GROUPS[j]

        def n_trip(k, _):
            for u in range(trip):
                n_group(first + 4 * (k * trip + u), slot)
            return 0
        lax.fori_loop(0, groups // trip, n_trip, 0)
        out_copy(t, slot).start()

    def block(b, _):
        @pl.when(lax.rem(b, COL_STEPS // ROW_STEPS) == 0)
        def _():
            col_exchange(lax.rem(b // (COL_STEPS // ROW_STEPS), 2))
        row_exchange(lax.rem(b, 2))
        for j in range(ROW_STEPS):
            one_step(b * ROW_STEPS + j, j)
        return 0
    lax.fori_loop(0, steps // ROW_STEPS, block, 0)

    def last_row(i, _):
        hlast[i] = H[HR + i][:, :tile_w]
        return 0
    lax.fori_loop(0, tile_h, last_row, 0)
    for t in (steps - 2, steps - 1):
        out_copy(t, t % 2).wait()


def split3(bias):
    top = float(jnp.finfo(BF).max)
    parts = []
    rest = bias
    for _ in range(3):
        part = jnp.clip(rest, -top, top).astype(BF)
        parts.append(part)
        rest = rest - part.astype(F32)
    return jnp.stack(parts, axis=1)


def prepare_weights(w_x, w_hzr, w_hn, gate_bias):
    ch = w_hn.shape[-1]
    cin = w_x.shape[2]
    half = jnp.asarray(0.5, BF)
    bias_zr = split3(0.5 * gate_bias[:2 * ch])
    wzr = jnp.concatenate([
        (w_hzr * half).reshape(9 * ch, 2 * ch).T,
        (w_x[..., :2 * ch] * half).reshape(9 * cin, 2 * ch).T,
        jnp.pad(bias_zr, ((0, 0), (0, 45)))], axis=1)
    wx_n = w_x[..., 2 * ch:]
    bias_n = jnp.pad(split3(gate_bias[2 * ch:]), ((0, 0), (0, 61)))
    halves = []
    for dy in range(2):
        pads = ((dy, 1 - dy), (0, 0), (0, 0), (0, 0))
        halves.append(jnp.concatenate([
            jnp.pad(w_hn, pads).reshape(12 * ch, ch).T,
            jnp.pad(wx_n, pads).reshape(12 * cin, ch).T,
            bias_n], axis=1))
    return wzr, jnp.concatenate(halves, axis=0)


def solution(mesh):
    n_rows = mesh.shape['rows']
    n_cols = mesh.shape['cols']
    frame_spec = P(None, 'batch', 'rows', 'cols', None)
    state_spec = P('batch', 'rows', 'cols', None)
    down_pairs = [(i, i + 1) for i in range(n_rows - 1)]
    up_pairs = [(i + 1, i) for i in range(n_rows - 1)]
    right_pairs = [(i, i + 1) for i in range(n_cols - 1)]
    left_pairs = [(i + 1, i) for i in range(n_cols - 1)]

    def local_fn(frames, h_init, w_x, w_hzr, w_hn, gate_bias):
        steps, _, tile_h, tile_w, cin = frames.shape
        ch = h_init.shape[-1]
        fr = frames[:, 0].transpose(0, 1, 3, 2)
        from_left = lax.ppermute(fr[..., tile_w - HC:], 'cols', right_pairs)
        from_right = lax.ppermute(fr[..., :HC], 'cols', left_pairs)
        gap = jnp.zeros(fr.shape[:-1] + (LANES - tile_w - 2 * HC,), BF)
        fr = jnp.concatenate([fr, from_right, gap, from_left], axis=-1)
        above = lax.ppermute(fr[:, tile_h - HR:], 'rows', down_pairs)
        below = lax.ppermute(fr[:, :HR], 'rows', up_pairs)
        fp = jnp.concatenate([above, fr, below], axis=1)
        wzr, wn = prepare_weights(w_x, w_hzr, w_hn, gate_bias)
        total_rows = tile_h + 2 * HR
        groups = tile_h * HC // LANES
        vmem = pl.BlockSpec(memory_space=pltpu.VMEM)
        anys = pl.BlockSpec(memory_space=pl.ANY)
        seq, last = pl.pallas_call(
            functools.partial(kernel, n_rows, n_cols),
            out_shape=(jax.ShapeDtypeStruct((steps, tile_h, ch, tile_w), BF),
                       jax.ShapeDtypeStruct((tile_h, ch, tile_w), F32)),
            in_specs=[anys, vmem, vmem, vmem],
            out_specs=(anys, vmem),
            scratch_shapes=[
                pltpu.VMEM((total_rows, ch, LANES), F32),
                pltpu.VMEM((total_rows * 3 * ch, LANES), BF),
                pltpu.VMEM((total_rows * 3 * ch, LANES), BF),
                pltpu.VMEM((total_rows * 3 * cin, LANES), BF),
                pltpu.VMEM((total_rows, ch, LANES), F32),
                pltpu.VMEM((2, total_rows, cin, LANES), BF),
                pltpu.VMEM((2, tile_h + 2 * ROW_STEPS, ch, tile_w), BF),
                pltpu.VMEM((2, groups, ch, LANES), F32),
                pltpu.VMEM((2, 2, groups, ch, LANES), F32),
                pltpu.VMEM((2, 2, HR, ch, LANES), F32),
                pltpu.SemaphoreType.DMA((2,)),
                pltpu.SemaphoreType.DMA((2,)),
                pltpu.SemaphoreType.DMA((2,)),
                pltpu.SemaphoreType.DMA((2, 2)),
                pltpu.SemaphoreType.DMA((2,)),
                pltpu.SemaphoreType.DMA((2, 2)),
            ],
            compiler_params=pltpu.CompilerParams(collective_id=0, has_side_effects=True, vmem_limit_bytes=60 * 1024 * 1024),
        )(fp, h_init[0].transpose(0, 2, 1), wzr, wn)
        return seq.transpose(0, 1, 3, 2)[:, None], last.transpose(0, 2, 1)[None]

    return jax.shard_map(local_fn, mesh=mesh, in_specs=(frame_spec, state_spec, P(), P(), P(), P()), out_specs=(frame_spec, state_spec), check_vma=False)
```

```python
import functools

import jax
import jax.numpy as jnp
from jax import lax
from jax.experimental import pallas as pl
from jax.experimental.pallas import tpu as pltpu
from jax.sharding import PartitionSpec as P

MESH = pl.DeviceIdType.MESH
LANES = 128
BF = jnp.bfloat16
F32 = jnp.float32

ROW_STEPS = 2
HR = 2 * ROW_STEPS
HC = 8
COL_STEPS = HC // 2
VMEM_MIB = 22
PER = LANES // HC


def store3(buf, base, size, val):
    buf[pl.ds(base, size), :] = pltpu.roll(val, 1, 1)
    buf[pl.ds(base + size, size), :] = val
    buf[pl.ds(base + 2 * size, size), :] = pltpu.roll(val, LANES - 1, 1)


def spin(val, shift):
    shift = shift % LANES
    return pltpu.roll(val, shift, 1) if shift else val


def kernel(n_rows, n_cols, frames, h0, wzr, wn, out, hlast,
           H, HB, RB, XB, Z, FS, XF, FC, FR, CS, CR, DR, RS, RR,
           fs_sem, fc_send, fc_recv, fh_send, fh_recv,
           cs_send, cs_recv, dg_send, dg_recv, rr_send, rr_recv):
    steps, tile_h, ch, tile_w = out.shape
    cin = frames.shape[2]
    total_rows = tile_h + 2 * HR
    n_slots = tile_w // HC
    n_groups = tile_h // PER
    n_blocks = steps // ROW_STEPS
    n_supers = steps // COL_STEPS
    per_super = COL_STEPS // ROW_STEPS
    row = lax.axis_index('rows')
    col = lax.axis_index('cols')
    has_v = (row > 0, row < n_rows - 1)
    has_h = (col > 0, col < n_cols - 1)
    diag = [(v, h, jnp.logical_and(has_v[v], has_h[h])) for v in range(2) for h in range(2)]

    def v_dev(v):
        return {'rows': row + 2 * v - 1}

    def h_dev(h):
        return {'cols': col + 2 * h - 1}

    def remote(src, dst, send, recv, dev):
        return pltpu.make_async_remote_copy(src, dst, send, recv, device_id=dev, device_id_type=MESH)

    def when_do(cond, fn):
        pl.when(cond)(fn)

    lane = lax.broadcasted_iota(jnp.int32, (ch, LANES), 1)
    slot_of = lane // HC
    lane_x = lax.broadcasted_iota(jnp.int32, (cin, LANES), 1)
    slot_x = lane_x // HC
    middle = (tile_w + HC + LANES - HC) // 2
    ones = jnp.where(lax.broadcasted_iota(jnp.int32, (64, LANES), 0) < 3, 1.0, 0.0).astype(BF)
    ok = [jnp.where(c, 1, 0) for c in has_v + has_h]
    lane_ok = jnp.where(lane < tile_w, 1, jnp.where(lane < tile_w + HC, ok[3], jnp.where(lane >= LANES - HC, ok[2], 0)))

    def frame_load(s):
        return pltpu.make_async_copy(frames.at[pl.ds(s * COL_STEPS, COL_STEPS)], FS, fs_sem)

    def frame_col(h, xslot):
        return remote(FC.at[h], FR.at[xslot, 1 - h], fc_send.at[h], fc_recv.at[xslot, 1 - h], h_dev(h))

    def frame_row(v, xslot):
        src = XF.at[xslot, :, pl.ds(HR + v * (tile_h - HR), HR)]
        dst = XF.at[xslot, :, pl.ds((1 - v) * (tile_h + HR), HR)]
        return remote(src, dst, fh_send.at[v], fh_recv.at[xslot, 1 - v], v_dev(v))

    def frames_pack(s):
        xslot = lax.rem(s, 2)
        frame_load(s).wait()

        def body(k, _):
            t = k // n_groups
            g = lax.rem(k, n_groups)
            left = jnp.zeros((cin, LANES), F32)
            right = jnp.zeros((cin, LANES), F32)
            for q in range(PER):
                r = g * PER + q
                XF[xslot, t, HR + r, :, 0:tile_w] = FS[t, r]
                moved = spin(XF[xslot, t, HR + r].astype(F32), HC * q)
                left = jnp.where(slot_x == q, moved, left)
                right = jnp.where(slot_x == (n_slots - 1 + q) % PER, moved, right)
            FC[0, t, g] = left.astype(BF)
            FC[1, t, g] = right.astype(BF)
            return 0
        lax.fori_loop(0, COL_STEPS * n_groups, body, 0)

        @pl.when(s + 1 < n_supers)
        def _():
            frame_load(s + 1).start()
        for h in range(2):
            when_do(has_h[h], frame_col(h, xslot).start)

    def frames_merge(s):
        xslot = lax.rem(s, 2)
        for h in range(2):
            when_do(has_h[h], frame_col(h, xslot).wait_send)
            when_do(has_h[h], frame_col(1 - h, xslot).wait_recv)

        def body(k, _):
            t = k // n_groups
            g = lax.rem(k, n_groups)
            from_right = FR[xslot, 1, t, g].astype(F32)
            from_left = FR[xslot, 0, t, g].astype(F32)
            for q in range(PER):
                r = g * PER + q
                right = spin(from_right, HC * (n_slots - q))
                left = spin(from_left, HC * (PER - n_slots - q))
                mine = XF[xslot, t, HR + r].astype(F32)
                XF[xslot, t, HR + r] = jnp.where(lane_x < tile_w, mine, jnp.where(lane_x < middle, right, left)).astype(BF)
            return 0
        lax.fori_loop(0, COL_STEPS * n_groups, body, 0)
        for v in range(2):
            when_do(has_v[v], frame_row(v, xslot).start)

    def frames_done(s):
        xslot = lax.rem(s, 2)
        for v in range(2):
            when_do(has_v[v], frame_row(v, xslot).wait_send)
            when_do(has_v[v], frame_row(1 - v, xslot).wait_recv)

    def col_copy(h, g, slot):
        return remote(CS.at[h, g], CR.at[slot, 1 - h, g], cs_send.at[h, g], cs_recv.at[slot, 1 - h, g], h_dev(h))

    def diag_copy(v, h, slot):
        g = 0 if v == 0 else n_groups - 1
        return remote(CS.at[h, g], DR.at[slot, 1 - v, 1 - h], dg_send.at[v, h], dg_recv.at[slot, 1 - v, 1 - h], {**v_dev(v), **h_dev(h)})

    def row_copy(v, slot):
        return remote(RS.at[v], RR.at[slot, 1 - v], rr_send.at[v], rr_recv.at[slot, 1 - v], v_dev(v))

    def col_send(g, slot):
        left = jnp.zeros((ch, LANES), F32)
        right = jnp.zeros((ch, LANES), F32)
        for q in range(PER):
            moved = spin(H[HR + g * PER + q], HC * q)
            left = jnp.where(slot_of == q, moved, left)
            right = jnp.where(slot_of == (n_slots - 1 + q) % PER, moved, right)
        CS[0, g] = left
        CS[1, g] = right
        for v, h, cond in diag:
            if g == (0 if v == 0 else n_groups - 1):
                when_do(cond, diag_copy(v, h, slot).start)
        for h in range(2):
            when_do(has_h[h], col_copy(h, g, slot).start)

    def col_take(g, slot):
        for h in range(2):
            when_do(has_h[h], col_copy(h, g, slot).wait_send)
            when_do(has_h[h], col_copy(1 - h, g, slot).wait_recv)
        from_right = CR[slot, 1, g]
        from_left = CR[slot, 0, g]
        for q in range(PER):
            i = HR + g * PER + q
            right = spin(from_right, HC * (n_slots - q))
            left = spin(from_left, HC * (PER - n_slots - q))
            val = jnp.where(lane < tile_w, H[i], jnp.where(lane < middle, right, left))
            H[i] = val
            store3(HB, i * 3 * ch, ch, val.astype(BF))

    def row_send(slot):
        RS[0] = H[HR:2 * HR]
        RS[1] = H[tile_h:tile_h + HR]
        for v in range(2):
            when_do(has_v[v], row_copy(v, slot).start)

    def row_take(slot, fresh, cslot):
        for v in range(2):
            when_do(has_v[v], row_copy(v, slot).wait_send)
            when_do(has_v[v], row_copy(1 - v, slot).wait_recv)

        @pl.when(fresh)
        def _():
            for v, h, cond in diag:
                when_do(cond, diag_copy(v, h, cslot).wait_send)
                when_do(cond, diag_copy(1 - v, 1 - h, cslot).wait_recv)
        bound = jnp.where(fresh, tile_w, LANES)
        for v in range(2):
            for i in range(HR):
                at = i + v * (tile_h + HR)
                q = i if v else PER - HR + i
                right = spin(DR[cslot, v, 1], HC * (n_slots - q))
                left = spin(DR[cslot, v, 0], HC * (PER - n_slots - q))
                val = jnp.where(lane < bound, RR[slot, v, i], jnp.where(lane < middle, right, left))
                H[at] = val
                store3(HB, at * 3 * ch, ch, val.astype(BF))

    def zr_tile(i):
        cols = []
        for d in range(2):
            hb = HB[pl.ds((i + d - 1) * (3 * ch), 9 * ch), :]
            xb = XB[pl.ds((i + d - 1) * (3 * cin), 9 * cin), :]
            cols.append(jnp.concatenate([hb, xb, ones[:48]], axis=0))
        acc = jnp.dot(wzr[...], jnp.concatenate(cols, axis=1), preferred_element_type=F32)
        gates = jnp.tanh(acc)
        for d in range(2):
            Z[i + d] = gates[:ch, d * LANES:(d + 1) * LANES]
            reset = 0.5 * gates[ch:, d * LANES:(d + 1) * LANES] + 0.5
            store3(RB, (i + d) * (3 * ch), ch, (reset * H[i + d]).astype(BF))

    def zr_rows(first, last):
        for r in range(first, last, 2):
            zr_tile(HR + r)

    def n_group(t, i):
        cols = []
        for p in range(2):
            y = i + 2 * p - 1
            hb = RB[pl.ds(y * (3 * ch), 12 * ch), :]
            xb = XB[pl.ds(y * (3 * cin), 12 * cin), :]
            cols.append(jnp.concatenate([hb, xb, ones], axis=0))
        acc = jnp.dot(wn[...], jnp.concatenate(cols, axis=1), preferred_element_type=F32)
        cand = jnp.tanh(acc)
        for p in range(2):
            for dy in range(2):
                at = i + 2 * p + dy
                inside = HR <= at < HR + tile_h
                cand_row = cand[dy * ch:(dy + 1) * ch, p * LANES:(p + 1) * LANES]
                update = 0.5 * Z[at] + 0.5
                new = cand_row + update * (H[at] - cand_row)
                mask = lane_ok if inside else lane_ok * (ok[0] if at < HR else ok[1])
                new = jnp.where(mask != 0, new, 0.0)
                H[at] = new
                new_bf = new.astype(BF)
                store3(HB, at * (3 * ch), ch, new_bf)
                if inside:
                    out[t, at - HR] = new_bf[:, :tile_w]

    def n_rows_of(t, first, last):
        for r in range(first, last, 4):
            n_group(t, HR + r)

    def spread(xslot, k):
        def body(i, _):
            for u in range(8):
                store3(XB, pl.multiple_of((i * 8 + u) * (3 * cin), 3 * cin), cin, XF[xslot, k, i * 8 + u])
            return 0
        lax.fori_loop(0, total_rows // 8, body, 0)

    frame_load(0).start()

    def init_row(i, _):
        H[i] = jnp.zeros((ch, LANES), F32)
        H[i, :, 0:tile_w] = h0[i - HR]
        return 0
    lax.fori_loop(HR, HR + tile_h, init_row, 0)
    for s in range(2):
        for side in range(2):
            CR[s, side] = jnp.zeros(CR.shape[2:], F32)
            DR[s, side] = jnp.zeros(DR.shape[2:], F32)
            RR[s, side] = jnp.zeros(RR.shape[2:], F32)

            def clear(k, _, s=s, side=side):
                XF[s, k, pl.ds(side * (tile_h + HR), HR)] = jnp.zeros((HR, cin, LANES), BF)
                return 0
            lax.fori_loop(0, COL_STEPS, clear, 0)
            FR[s, side] = jnp.zeros(FR.shape[2:], BF)

    barrier = pltpu.get_barrier_semaphore()
    peers = [(has_v[v], v_dev(v)) for v in range(2)] + [(has_h[h], h_dev(h)) for h in range(2)]
    peers += [(cond, {**v_dev(v), **h_dev(h)}) for v, h, cond in diag]
    for cond, dev in peers:
        @pl.when(cond)
        def _(dev=dev):
            pl.semaphore_signal(barrier, inc=1, device_id=dev, device_id_type=MESH)
    pl.semaphore_wait(barrier, sum(jnp.where(cond, 1, 0) for cond, _ in peers))

    frames_pack(0)
    row_send(0)
    for g in range(n_groups):
        col_send(g, 0)
    frames_merge(0)

    cuts = [PER * g - 1 if g else 1 for g in range(n_groups)] + [tile_h - 1]

    def block(b, _):
        s = b // per_super
        xslot = lax.rem(s, 2)
        in_super = lax.rem(b, per_super)
        fresh = in_super == 0
        t0 = b * ROW_STEPS
        k0 = in_super * ROW_STEPS

        @pl.when(fresh)
        def _():
            frames_done(s)

            @pl.when(s + 1 < n_supers)
            def _():
                frames_pack(s + 1)

        @pl.when(jnp.logical_and(in_super == per_super - 1, s + 1 < n_supers))
        def _():
            frames_merge(s + 1)

        spread(xslot, k0)
        for g in range(n_groups):
            @pl.when(fresh)
            def _(g=g):
                col_take(g, xslot)
            zr_rows(cuts[g], cuts[g + 1])
        row_take(lax.rem(b, 2), fresh, xslot)
        zr_rows(-3, 1)
        zr_rows(tile_h - 1, tile_h + 3)
        n_rows_of(t0, -2, tile_h + 2)

        spread(xslot, k0 + 1)
        zr_rows(-1, 5)
        zr_rows(tile_h - 5, tile_h + 1)
        n_rows_of(t0 + 1, 0, 4)
        n_rows_of(t0 + 1, tile_h - 4, tile_h)

        @pl.when(b + 1 < n_blocks)
        def _():
            row_send(lax.rem(b + 1, 2))
        zr_rows(5, tile_h - 5)
        send_cols = jnp.logical_and(in_super == per_super - 1, s + 1 < n_supers)
        for g in range(n_groups):
            n_rows_of(t0 + 1, max(PER * g, 4), min(PER * (g + 1), tile_h - 4))

            @pl.when(send_cols)
            def _(g=g):
                col_send(g, 1 - xslot)
        return 0
    lax.fori_loop(0, n_blocks, block, 0)

    def last_row(i, _):
        hlast[i] = H[HR + i][:, :tile_w]
        return 0
    lax.fori_loop(0, tile_h, last_row, 0)


def split3(bias):
    top = float(jnp.finfo(BF).max)
    parts = []
    rest = bias
    for _ in range(3):
        part = jnp.clip(rest, -top, top).astype(BF)
        parts.append(part)
        rest = rest - part.astype(F32)
    return jnp.stack(parts, axis=1)


def prepare_weights(w_x, w_hzr, w_hn, gate_bias):
    ch = w_hn.shape[-1]
    cin = w_x.shape[2]
    half = jnp.asarray(0.5, BF)
    bias_zr = split3(0.5 * gate_bias[:2 * ch])
    wzr = jnp.concatenate([
        (w_hzr * half).reshape(9 * ch, 2 * ch).T,
        (w_x[..., :2 * ch] * half).reshape(9 * cin, 2 * ch).T,
        jnp.pad(bias_zr, ((0, 0), (0, 45)))], axis=1)
    wx_n = w_x[..., 2 * ch:]
    bias_n = jnp.pad(split3(gate_bias[2 * ch:]), ((0, 0), (0, 61)))
    halves = []
    for dy in range(2):
        pads = ((dy, 1 - dy), (0, 0), (0, 0), (0, 0))
        halves.append(jnp.concatenate([
            jnp.pad(w_hn, pads).reshape(12 * ch, ch).T,
            jnp.pad(wx_n, pads).reshape(12 * cin, ch).T,
            bias_n], axis=1))
    return wzr, jnp.concatenate(halves, axis=0)


def solution(mesh):
    n_rows = mesh.shape['rows']
    n_cols = mesh.shape['cols']
    frame_spec = P(None, 'batch', 'rows', 'cols', None)
    state_spec = P('batch', 'rows', 'cols', None)

    def local_fn(frames, h_init, w_x, w_hzr, w_hn, gate_bias):
        steps, _, tile_h, tile_w, cin = frames.shape
        ch = h_init.shape[-1]
        wzr, wn = prepare_weights(w_x, w_hzr, w_hn, gate_bias)
        total_rows = tile_h + 2 * HR
        groups = tile_h // PER
        vmem = pl.BlockSpec(memory_space=pltpu.VMEM)
        anys = pl.BlockSpec(memory_space=pl.ANY)
        dma = pltpu.SemaphoreType.DMA
        seq, last = pl.pallas_call(
            functools.partial(kernel, n_rows, n_cols),
            out_shape=(jax.ShapeDtypeStruct((steps, tile_h, ch, tile_w), BF),
                       jax.ShapeDtypeStruct((tile_h, ch, tile_w), F32)),
            in_specs=[anys, vmem, vmem, vmem],
            out_specs=(vmem, vmem),
            scratch_shapes=[
                pltpu.VMEM((total_rows, ch, LANES), F32),
                pltpu.VMEM((total_rows * 3 * ch, LANES), BF),
                pltpu.VMEM((total_rows * 3 * ch, LANES), BF),
                pltpu.VMEM((total_rows * 3 * cin, LANES), BF),
                pltpu.VMEM((total_rows, ch, LANES), F32),
                pltpu.VMEM((COL_STEPS, tile_h, cin, tile_w), BF),
                pltpu.VMEM((2, COL_STEPS, total_rows, cin, LANES), BF),
                pltpu.VMEM((2, COL_STEPS, groups, cin, LANES), BF),
                pltpu.VMEM((2, 2, COL_STEPS, groups, cin, LANES), BF),
                pltpu.VMEM((2, groups, ch, LANES), F32),
                pltpu.VMEM((2, 2, groups, ch, LANES), F32),
                pltpu.VMEM((2, 2, 2, ch, LANES), F32),
                pltpu.VMEM((2, HR, ch, LANES), F32),
                pltpu.VMEM((2, 2, HR, ch, LANES), F32),
                dma(()), dma((2,)), dma((2, 2)), dma((2,)), dma((2, 2)),
                dma((2, groups)), dma((2, 2, groups)), dma((2, 2)), dma((2, 2, 2)), dma((2,)), dma((2, 2)),
            ],
            compiler_params=pltpu.CompilerParams(collective_id=0, has_side_effects=True, vmem_limit_bytes=VMEM_MIB * 1024 * 1024),
        )(frames[:, 0].transpose(0, 1, 3, 2), h_init[0].transpose(0, 2, 1), wzr, wn)
        return seq.transpose(0, 1, 3, 2)[:, None], last.transpose(0, 2, 1)[None]

    return jax.shard_map(local_fn, mesh=mesh, in_specs=(frame_spec, state_spec, P(), P(), P(), P()), out_specs=(frame_spec, state_spec), check_vma=False)
```

```python
import functools

import jax
import jax.numpy as jnp
from jax import lax
from jax.experimental import pallas as pl
from jax.experimental.pallas import tpu as pltpu
from jax.sharding import PartitionSpec as P

MESH = pl.DeviceIdType.MESH
LANES = 128
BF = jnp.bfloat16
F32 = jnp.float32

ROW_STEPS = 2
HR = 2 * ROW_STEPS
HC = 8
COL_STEPS = HC // 2
VMEM_MIB = 22
PER = LANES // HC


def store3(buf, base, size, val):
    buf[pl.ds(base, size), :] = pltpu.roll(val, 1, 1)
    buf[pl.ds(base + size, size), :] = val
    buf[pl.ds(base + 2 * size, size), :] = pltpu.roll(val, LANES - 1, 1)


def spin(val, shift):
    shift = shift % LANES
    return pltpu.roll(val, shift, 1) if shift else val


def kernel(n_rows, n_cols, frames, h0, w_x, w_hzr, w_hn, bias, out, hlast,
           H, HB, RB, XB, Z, KM, WZR, WN, HI, FS, XF, FC, FR, CS, CR, DS, DR, RS, RR,
           hi_sem, fs_sem, fc_send, fc_recv, fh_send, fh_recv,
           cs_send, cs_recv, dg_send, dg_recv, rr_send, rr_recv):
    steps, tile_h, ch, tile_w = out.shape
    cin = frames.shape[2]
    total_rows = tile_h + 2 * HR
    n_slots = tile_w // HC
    n_groups = tile_h // PER
    n_supers = steps // COL_STEPS
    per_super = COL_STEPS // ROW_STEPS
    row = lax.axis_index('rows')
    col = lax.axis_index('cols')
    has_v = (row > 0, row < n_rows - 1)
    has_h = (col > 0, col < n_cols - 1)
    diag = [(v, h, jnp.logical_and(has_v[v], has_h[h])) for v in range(2) for h in range(2)]

    def v_dev(v):
        return {'rows': row + 2 * v - 1}

    def h_dev(h):
        return {'cols': col + 2 * h - 1}

    def remote(src, dst, send, recv, dev):
        return pltpu.make_async_remote_copy(src, dst, send, recv, device_id=dev, device_id_type=MESH)

    def when_do(cond, *fns):
        @pl.when(cond)
        def _():
            for fn in fns:
                fn()

    lane = lax.broadcasted_iota(jnp.int32, (ch, LANES), 1)
    slot_of = lane // HC
    lane_x = lax.broadcasted_iota(jnp.int32, (cin, LANES), 1)
    slot_x = lane_x // HC
    middle = (tile_w + HC + LANES - HC) // 2
    ones = jnp.where(lax.broadcasted_iota(jnp.int32, (64, LANES), 0) < 3, 1.0, 0.0).astype(BF)
    ok = [jnp.where(c, 1, 0) for c in has_v + has_h]
    lane_ok = jnp.where(lane < tile_w, 1, jnp.where(lane < tile_w + HC, ok[3], jnp.where(lane >= LANES - HC, ok[2], 0)))
    lead = n_slots - 1

    def pack_rows(rows, slots, dtype):
        acc = [jnp.zeros(rows[0].shape, dtype), jnp.zeros(rows[0].shape, dtype)]
        for q, val in enumerate(rows):
            here = jnp.logical_or(slots == q, slots == (lead + q) % PER)
            acc[q % 2] = jnp.where(here, spin(val, HC * q), acc[q % 2])
        even = slots % 2 == 0
        return jnp.where(even, acc[0], acc[1]), jnp.where(even, acc[1], acc[0])

    def halo_rows(from_left, from_right, slots):
        turned = spin(from_left, HC * (3 - lead))
        even = slots % 2 == 0
        mixed = (jnp.where(even, from_right, turned), jnp.where(even, turned, from_right))
        return [spin(mixed[q % 2], HC * (n_slots - q)) for q in range(PER)]

    def frame_load(s):
        return pltpu.make_async_copy(frames.at[pl.ds(s * COL_STEPS, COL_STEPS)], FS, fs_sem)

    def frame_col(h, xslot):
        return remote(FC.at[h], FR.at[xslot, 1 - h], fc_send.at[h], fc_recv.at[xslot, 1 - h], h_dev(h))

    def frame_row(v, xslot):
        src = XF.at[xslot, :, pl.ds(HR + v * (tile_h - HR), HR)]
        dst = XF.at[xslot, :, pl.ds((1 - v) * (tile_h + HR), HR)]
        return remote(src, dst, fh_send.at[v], fh_recv.at[xslot, 1 - v], v_dev(v))

    def frames_pack(xslot, t):
        for g in range(n_groups):
            rows = []
            for q in range(PER):
                r = g * PER + q
                XF[xslot, t, HR + r, :, 0:tile_w] = FS[t, r]
                rows.append(XF[xslot, t, HR + r])
            FC[0, t, g], FC[1, t, g] = pack_rows(rows, slot_x, BF)

    def frames_merge(xslot, t):
        for g in range(n_groups):
            halos = halo_rows(FR[xslot, 0, t, g], FR[xslot, 1, t, g], slot_x)
            for q in range(PER):
                r = HR + g * PER + q
                XF[xslot, t, r] = jnp.where(lane_x < tile_w, XF[xslot, t, r], halos[q])

    def frames_cols_wait(xslot, cond):
        for h in range(2):
            when_do(jnp.logical_and(cond, has_h[h]), frame_col(h, xslot).wait_send, frame_col(1 - h, xslot).wait_recv)

    def frames_rows_wait(xslot):
        for v in range(2):
            when_do(has_v[v], frame_row(v, xslot).wait_send, frame_row(1 - v, xslot).wait_recv)

    def spread(xslot, k, first, last):
        for i in range(first, last):
            store3(XB, ((k % 2) * total_rows + i) * (3 * cin), cin, XF[xslot, k, i])

    def col_copy(h, g, slot):
        return remote(CS.at[h, g], CR.at[slot, 1 - h, g], cs_send.at[h, g], cs_recv.at[slot, 1 - h, g], h_dev(h))

    def diag_copy(v, h, slot):
        return remote(DS.at[v, h], DR.at[slot, 1 - v, 1 - h], dg_send.at[v, h], dg_recv.at[slot, 1 - v, 1 - h], {**v_dev(v), **h_dev(h)})

    def row_copy(v, slot):
        return remote(RS.at[v], RR.at[slot, 1 - v], rr_send.at[v], rr_recv.at[slot, 1 - v], v_dev(v))

    wide = HR * HC
    quarter = lax.broadcasted_iota(jnp.int32, (ch * wide // LANES, LANES), 1) // wide
    parts = LANES // wide
    part_ch = ch // parts

    def col_send(g, slot, cond):
        edges = pack_rows([H[HR + g * PER + q] for q in range(PER)], slot_of, F32)
        for h in range(2):
            CS[h, g] = edges[h]
        for v in range(2):
            if g == (0 if v == 0 else n_groups - 1):
                for h in range(2):
                    first = (0 if v == 0 else PER - HR) + h * lead
                    small = jnp.zeros((part_ch, LANES), F32)
                    for c in range(parts):
                        small = jnp.where(quarter == c, spin(edges[h][c * part_ch:(c + 1) * part_ch], wide * c - HC * first), small)
                    DS[v, h] = small
        for h in range(2):
            when_do(jnp.logical_and(cond, has_h[h]), col_copy(h, g, slot).start)
        for v, h, both in diag:
            if g == (0 if v == 0 else n_groups - 1):
                when_do(jnp.logical_and(cond, both), diag_copy(v, h, slot).start)

    def col_take(g, slot):
        for h in range(2):
            when_do(has_h[h], col_copy(h, g, slot).wait_send, col_copy(1 - h, g, slot).wait_recv)
        halos = halo_rows(CR[slot, 0, g], CR[slot, 1, g], slot_of)
        for q in range(PER):
            i = HR + g * PER + q
            val = jnp.where(lane < tile_w, H[i], halos[q])
            H[i] = val
            store3(HB, i * 3 * ch, ch, val.astype(BF))

    def row_send(slot, cond):
        RS[0] = H[HR:2 * HR]
        RS[1] = H[tile_h:tile_h + HR]
        for v in range(2):
            when_do(jnp.logical_and(cond, has_v[v]), row_copy(v, slot).start)

    def row_take(slot, fresh, cslot):
        for v in range(2):
            when_do(has_v[v], row_copy(v, slot).wait_send, row_copy(1 - v, slot).wait_recv)
        if fresh:
            for v, h, cond in diag:
                when_do(cond, diag_copy(v, h, cslot).wait_send, diag_copy(1 - v, 1 - h, cslot).wait_recv)
        for v in range(2):
            for i in range(HR):
                at = i + v * (tile_h + HR)
                val = RR[slot, v, i]
                if fresh:
                    sides = []
                    for h, to in ((0, LANES - HC), (1, tile_w)):
                        small = DR[cslot, v, h]
                        sides.append(jnp.concatenate([spin(small, to - wide * c - HC * i) for c in range(parts)], axis=0))
                    val = jnp.where(lane < tile_w, val, jnp.where(lane < middle, sides[1], sides[0]))
                H[at] = val
                store3(HB, at * 3 * ch, ch, val.astype(BF))

    def frame_rows(k, i, count):
        return XB[pl.ds(((k % 2) * total_rows + i) * (3 * cin), count * 3 * cin), :]

    def zr_rows(k, first, last):
        for r in range(first, last, 2):
            i = HR + r
            cols = []
            for d in range(2):
                hb = HB[pl.ds((i + d - 1) * (3 * ch), 9 * ch), :]
                cols.append(jnp.concatenate([hb, frame_rows(k, i + d - 1, 3), ones[:48]], axis=0))
            acc = jnp.dot(WZR[...], jnp.concatenate(cols, axis=1), preferred_element_type=F32)
            gates = jnp.tanh(acc)
            for d in range(2):
                Z[i + d] = gates[:ch, d * LANES:(d + 1) * LANES]
                reset = 0.5 * gates[ch:, d * LANES:(d + 1) * LANES] + 0.5
                store3(RB, (i + d) * (3 * ch), ch, (reset * H[i + d]).astype(BF))

    def n_rows_of(t, k, first, last, keep):
        for r in range(first, last, 4):
            i = HR + r
            cols = []
            for p in range(2):
                y = i + 2 * p - 1
                cols.append(jnp.concatenate([RB[pl.ds(y * (3 * ch), 12 * ch), :], frame_rows(k, y, 4), ones], axis=0))
            acc = jnp.dot(WN[...], jnp.concatenate(cols, axis=1), preferred_element_type=F32)
            cand = jnp.tanh(acc)
            for p in range(2):
                for dy in range(2):
                    at = i + 2 * p + dy
                    inside = HR <= at < HR + tile_h
                    cand_row = cand[dy * ch:(dy + 1) * ch, p * LANES:(p + 1) * LANES]
                    update = 0.5 * Z[at] + 0.5
                    new = cand_row + update * (H[at] - cand_row)
                    mask = lane_ok if inside else lane_ok * (ok[0] if at < HR else ok[1])
                    new = jnp.where(mask != 0, new, 0.0)
                    H[at] = new
                    new_bf = new.astype(BF)
                    if keep:
                        store3(HB, at * (3 * ch), ch, new_bf)
                    if inside:
                        out[t, at - HR] = new_bf[:, :tile_w]

    def prepare_weights():
        def split3(val):
            top = float(jnp.finfo(BF).max)
            parts3 = []
            for _ in range(3):
                part = jnp.clip(val, -top, top).astype(BF).astype(F32)
                parts3.append(part)
                val = val - part
            return parts3

        def bias_rows(vals, count):
            at = lax.broadcasted_iota(jnp.int32, (count, LANES), 0)
            rows = jnp.zeros((count, LANES), F32)
            for n, part in enumerate(split3(vals)):
                rows = jnp.where(at == n, jnp.broadcast_to(part, (count, LANES)), rows)
            return rows

        def turn(dst):
            for c in range(dst.shape[1] // LANES):
                dst[:, c * LANES:(c + 1) * LANES] = KM[c * LANES:(c + 1) * LANES, :].T.astype(BF)

        taps, xtaps = 9 * ch, 9 * cin
        KM[0:taps] = 0.5 * w_hzr[...].astype(F32)
        KM[taps:taps + xtaps] = 0.5 * w_x[:, 0:2 * ch].astype(F32)
        KM[taps + xtaps:taps + xtaps + 48] = bias_rows(0.5 * bias[:, 0:2 * ch], 48)
        turn(WZR)

        def both(w, step):
            gap = jnp.zeros((step, ch), F32)
            return jnp.concatenate([jnp.concatenate([w, gap], axis=0), jnp.concatenate([gap, w], axis=0)], axis=1)
        KM[0:12 * ch] = both(w_hn[...].astype(F32), 3 * ch)
        KM[12 * ch:12 * ch + 12 * cin] = both(w_x[:, 2 * ch:3 * ch].astype(F32), 3 * cin)
        bias_n = bias[:, 2 * ch:3 * ch]
        KM[12 * ch + 12 * cin:12 * ch + 12 * cin + 64] = bias_rows(jnp.concatenate([bias_n, bias_n], axis=1), 64)
        turn(WN)

    frame_load(0).start()
    h_load = pltpu.make_async_copy(h0, HI, hi_sem)
    h_load.start()
    for s in range(2):
        for side in range(2):
            CR[s, side] = jnp.zeros(CR.shape[2:], F32)
            DR[s, side] = jnp.zeros(DR.shape[2:], F32)
            RR[s, side] = jnp.zeros(RR.shape[2:], F32)
            FR[s, side] = jnp.zeros(FR.shape[2:], BF)
            for k in range(COL_STEPS):
                XF[s, k, pl.ds(side * (tile_h + HR), HR)] = jnp.zeros((HR, cin, LANES), BF)

    barrier = pltpu.get_barrier_semaphore()
    peers = [(has_v[v], v_dev(v)) for v in range(2)] + [(has_h[h], h_dev(h)) for h in range(2)]
    peers += [(cond, {**v_dev(v), **h_dev(h)}) for v, h, cond in diag]
    for cond, dev in peers:
        @pl.when(cond)
        def _(dev=dev):
            pl.semaphore_signal(barrier, inc=1, device_id=dev, device_id_type=MESH)
    h_load.wait()

    def init_row(i, _):
        H[i] = jnp.zeros((ch, LANES), F32)
        H[i, :, 0:tile_w] = HI[i - HR]
        return 0
    lax.fori_loop(HR, HR + tile_h, init_row, 0)
    frame_load(0).wait()
    for t in range(COL_STEPS):
        frames_pack(0, t)
    frame_load(1).start()
    pl.semaphore_wait(barrier, sum(jnp.where(cond, 1, 0) for cond, _ in peers))
    for h in range(2):
        when_do(has_h[h], frame_col(h, 0).start)
    row_send(0, True)
    for g in range(n_groups):
        col_send(g, 0, True)
    prepare_weights()
    frames_cols_wait(0, True)
    for t in range(COL_STEPS):
        frames_merge(0, t)
    for v in range(2):
        when_do(has_v[v], frame_row(v, 0).start)
    spread(0, 0, HR, HR + tile_h)

    cuts = [PER * g - 1 if g else 1 for g in range(n_groups)] + [tile_h - 1]
    far = total_rows

    def super_block(s, _):
        xslot = lax.rem(s, 2)
        more = s + 1 < n_supers
        for bi in range(per_super):
            k = bi * ROW_STEPS
            t = s * COL_STEPS + k
            fresh = bi == 0
            ends = bi == per_super - 1
            if fresh:
                for g in range(n_groups):
                    col_take(g, xslot)
                    zr_rows(k, cuts[g], cuts[g + 1])
                frames_rows_wait(xslot)
                spread(xslot, 0, 0, HR)
                spread(xslot, 0, HR + tile_h, far)
            else:
                frames_cols_wait(1 - xslot, more)
                zr_rows(k, 1, tile_h - 1)
                for u in range(COL_STEPS):
                    frames_merge(1 - xslot, u)
                for v in range(2):
                    when_do(jnp.logical_and(more, has_v[v]), frame_row(v, 1 - xslot).start)
            row_take(bi % 2, fresh, xslot)
            zr_rows(k, -3, 1)
            zr_rows(k, tile_h - 1, tile_h + 3)
            n_rows_of(t, k, -2, tile_h + 2, True)
            spread(xslot, k + 1, 0, far)
            zr_rows(k + 1, -1, 5)
            zr_rows(k + 1, tile_h - 5, tile_h + 1)
            n_rows_of(t + 1, k + 1, 0, 4, not ends)
            n_rows_of(t + 1, k + 1, tile_h - 4, tile_h, not ends)
            if fresh:
                when_do(more, frame_load(s + 1).wait)
            row_send((bi + 1) % 2, more if ends else True)
            zr_rows(k + 1, 5, tile_h - 5)
            if fresh:
                for u in range(COL_STEPS):
                    frames_pack(1 - xslot, u)
            if ends:
                for g in range(n_groups):
                    n_rows_of(t + 1, k + 1, max(PER * g, 4), min(PER * (g + 1), tile_h - 4), False)
                    col_send(g, 1 - xslot, more)
                spread(1 - xslot, 0, HR, HR + tile_h)
            else:
                n_rows_of(t + 1, k + 1, 4, tile_h - 4, True)
                spread(xslot, k + 2, 0, far)
            if fresh:
                for h in range(2):
                    when_do(jnp.logical_and(more, has_h[h]), frame_col(h, 1 - xslot).start)
                when_do(s + 2 < n_supers, frame_load(s + 2).start)
        return 0
    lax.fori_loop(0, n_supers, super_block, 0)

    def last_row(i, _):
        hlast[i] = H[HR + i][:, :tile_w]
        return 0
    lax.fori_loop(0, tile_h, last_row, 0)


def solution(mesh):
    n_rows = mesh.shape['rows']
    n_cols = mesh.shape['cols']
    frame_spec = P(None, 'batch', 'rows', 'cols', None)
    state_spec = P('batch', 'rows', 'cols', None)

    def local_fn(frames, h_init, w_x, w_hzr, w_hn, gate_bias):
        steps, _, tile_h, tile_w, cin = frames.shape
        ch = h_init.shape[-1]
        total_rows = tile_h + 2 * HR
        groups = tile_h // PER
        vmem = pl.BlockSpec(memory_space=pltpu.VMEM)
        hbm = pl.BlockSpec(memory_space=pltpu.HBM)
        dma = pltpu.SemaphoreType.DMA
        corner = (ch * HR * HC // LANES, LANES)
        seq, last = pl.pallas_call(
            functools.partial(kernel, n_rows, n_cols),
            out_shape=(jax.ShapeDtypeStruct((steps, tile_h, ch, tile_w), BF),
                       jax.ShapeDtypeStruct((tile_h, ch, tile_w), F32)),
            in_specs=[hbm, hbm, vmem, vmem, vmem, vmem],
            out_specs=(vmem, vmem),
            scratch_shapes=[
                pltpu.VMEM((total_rows, ch, LANES), F32),
                pltpu.VMEM((total_rows * 3 * ch, LANES), BF),
                pltpu.VMEM((total_rows * 3 * ch, LANES), BF),
                pltpu.VMEM((2 * total_rows * 3 * cin, LANES), BF),
                pltpu.VMEM((total_rows, ch, LANES), F32),
                pltpu.VMEM((12 * ch + 12 * cin + 64, LANES), F32),
                pltpu.VMEM((2 * ch, 9 * ch + 9 * cin + 48), BF),
                pltpu.VMEM((2 * ch, 12 * ch + 12 * cin + 64), BF),
                pltpu.VMEM((tile_h, ch, tile_w), F32),
                pltpu.VMEM((COL_STEPS, tile_h, cin, tile_w), BF),
                pltpu.VMEM((2, COL_STEPS, total_rows, cin, LANES), BF),
                pltpu.VMEM((2, COL_STEPS, groups, cin, LANES), BF),
                pltpu.VMEM((2, 2, COL_STEPS, groups, cin, LANES), BF),
                pltpu.VMEM((2, groups, ch, LANES), F32),
                pltpu.VMEM((2, 2, groups, ch, LANES), F32),
                pltpu.VMEM((2, 2) + corner, F32),
                pltpu.VMEM((2, 2, 2) + corner, F32),
                pltpu.VMEM((2, HR, ch, LANES), F32),
                pltpu.VMEM((2, 2, HR, ch, LANES), F32),
                dma(()), dma(()), dma((2,)), dma((2, 2)), dma((2,)), dma((2, 2)),
                dma((2, groups)), dma((2, 2, groups)), dma((2, 2)), dma((2, 2, 2)), dma((2,)), dma((2, 2)),
            ],
            compiler_params=pltpu.CompilerParams(collective_id=0, has_side_effects=True, vmem_limit_bytes=VMEM_MIB * 1024 * 1024),
        )(frames[:, 0].transpose(0, 1, 3, 2), h_init[0].transpose(0, 2, 1), w_x.reshape(9 * cin, 3 * ch),
          w_hzr.reshape(9 * ch, 2 * ch), w_hn.reshape(9 * ch, ch), gate_bias[None])
        return seq.transpose(0, 1, 3, 2)[:, None], last.transpose(0, 2, 1)[None]

    return jax.shard_map(local_fn, mesh=mesh, in_specs=(frame_spec, state_spec, P(), P(), P(), P()), out_specs=(frame_spec, state_spec), check_vma=False)
```

```python
import functools

import jax
import jax.numpy as jnp
from jax import lax
from jax.experimental import pallas as pl
from jax.experimental.pallas import tpu as pltpu
from jax.sharding import PartitionSpec as P

MESH = pl.DeviceIdType.MESH
LANES = 128
BF = jnp.bfloat16
F32 = jnp.float32

ROW_STEPS = 2
HR = 2 * ROW_STEPS
HC = 8
COL_STEPS = HC // 2
VMEM_MIB = 24
PER = LANES // HC


def store3(buf, base, size, val):
    buf[pl.ds(base, size), :] = pltpu.roll(val, 1, 1)
    buf[pl.ds(base + size, size), :] = val
    buf[pl.ds(base + 2 * size, size), :] = pltpu.roll(val, LANES - 1, 1)


def spin(val, shift):
    shift = shift % LANES
    return pltpu.roll(val, shift, 1) if shift else val


def kernel(n_rows, n_cols, frames, h0, w_x_in, w_hzr_in, w_hn_in, bias_in, out, hlast,
           H, HB, RB, XB, Z, KM, WZR, WN, HI, w_x, w_hzr, w_hn, bias, FS, XF, FC, FR, CS, CR, DS, DR, RS, RR,
           hi_sem, w_sem, fs_sem, fc_send, fc_recv, fh_send, fh_recv,
           cs_send, cs_recv, dg_send, dg_recv, rr_send, rr_recv):
    steps, tile_h, ch, tile_w = out.shape
    cin = frames.shape[2]
    total_rows = tile_h + 2 * HR
    n_slots = tile_w // HC
    n_groups = tile_h // PER
    n_supers = steps // COL_STEPS
    per_super = COL_STEPS // ROW_STEPS
    row = lax.axis_index('rows')
    col = lax.axis_index('cols')
    has_v = (row > 0, row < n_rows - 1)
    has_h = (col > 0, col < n_cols - 1)
    diag = [(v, h, jnp.logical_and(has_v[v], has_h[h])) for v in range(2) for h in range(2)]

    def v_dev(v):
        return {'rows': row + 2 * v - 1}

    def h_dev(h):
        return {'cols': col + 2 * h - 1}

    def remote(src, dst, send, recv, dev):
        return pltpu.make_async_remote_copy(src, dst, send, recv, device_id=dev, device_id_type=MESH)

    def when_do(cond, *fns):
        @pl.when(cond)
        def _():
            for fn in fns:
                fn()

    lane = lax.broadcasted_iota(jnp.int32, (ch, LANES), 1)
    slot_of = lane // HC
    lane_x = lax.broadcasted_iota(jnp.int32, (cin, LANES), 1)
    slot_x = lane_x // HC
    middle = (tile_w + HC + LANES - HC) // 2
    ones = jnp.where(lax.broadcasted_iota(jnp.int32, (64, LANES), 0) < 3, 1.0, 0.0).astype(BF)
    ok = [jnp.where(c, 1, 0) for c in has_v + has_h]
    lane_ok = jnp.where(lane < tile_w, 1, jnp.where(lane < tile_w + HC, ok[3], jnp.where(lane >= LANES - HC, ok[2], 0)))
    lead = n_slots - 1

    def pack_rows(rows, slots, dtype):
        acc = [jnp.zeros(rows[0].shape, dtype), jnp.zeros(rows[0].shape, dtype)]
        for q, val in enumerate(rows):
            here = jnp.logical_or(slots == q, slots == (lead + q) % PER)
            acc[q % 2] = jnp.where(here, spin(val, HC * q), acc[q % 2])
        even = slots % 2 == 0
        return jnp.where(even, acc[0], acc[1]), jnp.where(even, acc[1], acc[0])

    def halo_rows(from_left, from_right, slots):
        turned = spin(from_left, HC * (PER - 1 - n_slots - lead))
        even = slots % 2 == 0
        mixed = (jnp.where(even, from_right, turned), jnp.where(even, turned, from_right))
        return [spin(mixed[q % 2], HC * (n_slots - q)) for q in range(PER)]

    def frame_load(s):
        return pltpu.make_async_copy(frames.at[pl.ds(s * COL_STEPS, COL_STEPS)], FS, fs_sem)

    def frame_col(h, xslot):
        return remote(FC.at[h], FR.at[xslot, 1 - h], fc_send.at[h], fc_recv.at[xslot, 1 - h], h_dev(h))

    def frame_row(v, xslot):
        src = XF.at[xslot, :, pl.ds(HR + v * (tile_h - HR), HR)]
        dst = XF.at[xslot, :, pl.ds((1 - v) * (tile_h + HR), HR)]
        return remote(src, dst, fh_send.at[v], fh_recv.at[xslot, 1 - v], v_dev(v))

    def frames_pack(xslot, t):
        for g in range(n_groups):
            rows = []
            for q in range(PER):
                r = g * PER + q
                XF[xslot, t, HR + r, :, 0:tile_w] = FS[t, r]
                rows.append(XF[xslot, t, HR + r])
            FC[0, t, g], FC[1, t, g] = pack_rows(rows, slot_x, BF)

    def frames_merge(xslot, t):
        for g in range(n_groups):
            halos = halo_rows(FR[xslot, 0, t, g], FR[xslot, 1, t, g], slot_x)
            for q in range(PER):
                r = HR + g * PER + q
                XF[xslot, t, r] = jnp.where(lane_x < tile_w, XF[xslot, t, r], halos[q])

    def frames_cols_wait(xslot, cond):
        for h in range(2):
            when_do(jnp.logical_and(cond, has_h[h]), frame_col(h, xslot).wait_send, frame_col(1 - h, xslot).wait_recv)

    def frames_rows_wait(xslot):
        for v in range(2):
            when_do(has_v[v], frame_row(v, xslot).wait_send, frame_row(1 - v, xslot).wait_recv)

    def spread(xslot, k, first, last):
        for i in range(first, last):
            store3(XB, ((k % 2) * total_rows + i) * (3 * cin), cin, XF[xslot, k, i])

    def col_copy(h, g, slot):
        return remote(CS.at[h, g], CR.at[slot, 1 - h, g], cs_send.at[h, g], cs_recv.at[slot, 1 - h, g], h_dev(h))

    def diag_copy(v, h, slot):
        return remote(DS.at[v, h], DR.at[slot, 1 - v, 1 - h], dg_send.at[v, h], dg_recv.at[slot, 1 - v, 1 - h], {**v_dev(v), **h_dev(h)})

    def row_copy(v, slot):
        return remote(RS.at[v], RR.at[slot, 1 - v], rr_send.at[v], rr_recv.at[slot, 1 - v], v_dev(v))

    wide = HR * HC
    quarter = lax.broadcasted_iota(jnp.int32, (ch * wide // LANES, LANES), 1) // wide
    parts = LANES // wide
    part_ch = ch // parts

    def col_send(g, slot, cond):
        edges = pack_rows([H[HR + g * PER + q] for q in range(PER)], slot_of, F32)
        for h in range(2):
            CS[h, g] = edges[h]
        for v in range(2):
            if g == (0 if v == 0 else n_groups - 1):
                for h in range(2):
                    first = (0 if v == 0 else PER - HR) + h * lead
                    small = jnp.zeros((part_ch, LANES), F32)
                    for c in range(parts):
                        small = jnp.where(quarter == c, spin(edges[h][c * part_ch:(c + 1) * part_ch], wide * c - HC * first), small)
                    DS[v, h] = small
        for h in range(2):
            when_do(jnp.logical_and(cond, has_h[h]), col_copy(h, g, slot).start)
        for v, h, both in diag:
            if g == (0 if v == 0 else n_groups - 1):
                when_do(jnp.logical_and(cond, both), diag_copy(v, h, slot).start)

    def col_take(g, slot):
        for h in range(2):
            when_do(has_h[h], col_copy(h, g, slot).wait_send, col_copy(1 - h, g, slot).wait_recv)
        halos = halo_rows(CR[slot, 0, g], CR[slot, 1, g], slot_of)
        for q in range(PER):
            i = HR + g * PER + q
            val = jnp.where(lane < tile_w, H[i], halos[q])
            H[i] = val
            store3(HB, i * 3 * ch, ch, val.astype(BF))

    def row_send(slot, cond):
        RS[0] = H[HR:2 * HR]
        RS[1] = H[tile_h:tile_h + HR]
        for v in range(2):
            when_do(jnp.logical_and(cond, has_v[v]), row_copy(v, slot).start)

    def row_take(slot, fresh, cslot):
        for v in range(2):
            when_do(has_v[v], row_copy(v, slot).wait_send, row_copy(1 - v, slot).wait_recv)
        if fresh:
            for v, h, cond in diag:
                when_do(cond, diag_copy(v, h, cslot).wait_send, diag_copy(1 - v, 1 - h, cslot).wait_recv)
        for v in range(2):
            for i in range(HR):
                at = i + v * (tile_h + HR)
                val = RR[slot, v, i]
                if fresh:
                    sides = []
                    for h, to in ((0, LANES - HC), (1, tile_w)):
                        small = DR[cslot, v, h]
                        sides.append(jnp.concatenate([spin(small, to - wide * c - HC * i) for c in range(parts)], axis=0))
                    val = jnp.where(lane < tile_w, val, jnp.where(lane < middle, sides[1], sides[0]))
                H[at] = val
                store3(HB, at * 3 * ch, ch, val.astype(BF))

    def frame_rows(k, i, count):
        return XB[pl.ds(((k % 2) * total_rows + i) * (3 * cin), count * 3 * cin), :]

    def zr_rows(k, first, last):
        for r in range(first, last, 2):
            i = HR + r
            cols = []
            for d in range(2):
                hb = HB[pl.ds((i + d - 1) * (3 * ch), 9 * ch), :]
                cols.append(jnp.concatenate([hb, frame_rows(k, i + d - 1, 3), ones[:48]], axis=0))
            acc = jnp.dot(WZR[...], jnp.concatenate(cols, axis=1), preferred_element_type=F32)
            gates = jnp.tanh(acc)
            for d in range(2):
                Z[i + d] = gates[:ch, d * LANES:(d + 1) * LANES]
                reset = 0.5 * gates[ch:, d * LANES:(d + 1) * LANES] + 0.5
                store3(RB, (i + d) * (3 * ch), ch, (reset * H[i + d]).astype(BF))

    def n_rows_of(t, k, first, last, keep):
        for r in range(first, last, 4):
            i = HR + r
            cols = []
            for p in range(2):
                y = i + 2 * p - 1
                cols.append(jnp.concatenate([RB[pl.ds(y * (3 * ch), 12 * ch), :], frame_rows(k, y, 4), ones], axis=0))
            acc = jnp.dot(WN[...], jnp.concatenate(cols, axis=1), preferred_element_type=F32)
            cand = jnp.tanh(acc)
            for p in range(2):
                for dy in range(2):
                    at = i + 2 * p + dy
                    inside = HR <= at < HR + tile_h
                    cand_row = cand[dy * ch:(dy + 1) * ch, p * LANES:(p + 1) * LANES]
                    update = 0.5 * Z[at] + 0.5
                    new = cand_row + update * (H[at] - cand_row)
                    mask = lane_ok if inside else lane_ok * (ok[0] if at < HR else ok[1])
                    new = jnp.where(mask != 0, new, 0.0)
                    H[at] = new
                    new_bf = new.astype(BF)
                    if keep:
                        store3(HB, at * (3 * ch), ch, new_bf)
                    if inside:
                        out[t, at - HR] = new_bf[:, :tile_w]

    def prepare_weights():
        def split3(val):
            top = float(jnp.finfo(BF).max)
            parts3 = []
            for _ in range(3):
                part = jnp.clip(val, -top, top).astype(BF).astype(F32)
                parts3.append(part)
                val = val - part
            return parts3

        def bias_rows(vals, count):
            at = lax.broadcasted_iota(jnp.int32, (count, LANES), 0)
            rows = jnp.zeros((count, LANES), F32)
            for n, part in enumerate(split3(vals)):
                rows = jnp.where(at == n, jnp.broadcast_to(part, (count, LANES)), rows)
            return rows

        def turn(dst):
            for c in range(dst.shape[1] // LANES):
                dst[:, c * LANES:(c + 1) * LANES] = KM[c * LANES:(c + 1) * LANES, :].T.astype(BF)

        taps, xtaps = 9 * ch, 9 * cin
        KM[0:taps] = 0.5 * w_hzr[...].astype(F32)
        KM[taps:taps + xtaps] = 0.5 * w_x[:, 0:2 * ch].astype(F32)
        KM[taps + xtaps:taps + xtaps + 48] = bias_rows(0.5 * bias[:, 0:2 * ch], 48)
        turn(WZR)

        def both(w, step):
            gap = jnp.zeros((step, ch), F32)
            return jnp.concatenate([jnp.concatenate([w, gap], axis=0), jnp.concatenate([gap, w], axis=0)], axis=1)
        KM[0:12 * ch] = both(w_hn[...].astype(F32), 3 * ch)
        KM[12 * ch:12 * ch + 12 * cin] = both(w_x[:, 2 * ch:3 * ch].astype(F32), 3 * cin)
        bias_n = bias[:, 2 * ch:3 * ch]
        KM[12 * ch + 12 * cin:12 * ch + 12 * cin + 64] = bias_rows(jnp.concatenate([bias_n, bias_n], axis=1), 64)
        turn(WN)

    frame_load(0).start()
    h_load = pltpu.make_async_copy(h0, HI, hi_sem)
    h_load.start()
    w_loads = [pltpu.make_async_copy(src, dst, w_sem.at[n]) for n, (src, dst) in enumerate(
        ((w_x_in, w_x), (w_hzr_in, w_hzr), (w_hn_in, w_hn), (bias_in, bias)))]
    for load in w_loads:
        load.start()
    for s in range(2):
        for side in range(2):
            CR[s, side] = jnp.zeros(CR.shape[2:], F32)
            DR[s, side] = jnp.zeros(DR.shape[2:], F32)
            RR[s, side] = jnp.zeros(RR.shape[2:], F32)
            FR[s, side] = jnp.zeros(FR.shape[2:], BF)
            for k in range(COL_STEPS):
                XF[s, k, pl.ds(side * (tile_h + HR), HR)] = jnp.zeros((HR, cin, LANES), BF)

    barrier = pltpu.get_barrier_semaphore()
    peers = [(has_v[v], v_dev(v)) for v in range(2)] + [(has_h[h], h_dev(h)) for h in range(2)]
    peers += [(cond, {**v_dev(v), **h_dev(h)}) for v, h, cond in diag]
    for cond, dev in peers:
        @pl.when(cond)
        def _(dev=dev):
            pl.semaphore_signal(barrier, inc=1, device_id=dev, device_id_type=MESH)
    h_load.wait()

    def init_row(i, _):
        H[i] = jnp.zeros((ch, LANES), F32)
        H[i, :, 0:tile_w] = HI[i - HR]
        return 0
    lax.fori_loop(HR, HR + tile_h, init_row, 0)
    frame_load(0).wait()
    for t in range(COL_STEPS):
        frames_pack(0, t)
    frame_load(1).start()
    pl.semaphore_wait(barrier, sum(jnp.where(cond, 1, 0) for cond, _ in peers))
    for h in range(2):
        when_do(has_h[h], frame_col(h, 0).start)
    row_send(0, True)
    for g in range(n_groups):
        col_send(g, 0, True)
    for load in w_loads:
        load.wait()
    prepare_weights()
    frames_cols_wait(0, True)
    for t in range(COL_STEPS):
        frames_merge(0, t)
    for v in range(2):
        when_do(has_v[v], frame_row(v, 0).start)
    spread(0, 0, HR, HR + tile_h)

    cuts = [PER * g - 1 if g else 1 for g in range(n_groups)] + [tile_h - 1]
    far = total_rows

    if COL_STEPS == 4:
        packs, merges = {0: [0, 1], 1: [2, 3]}, {3: [0, 1, 2, 3]}
    else:
        packs, merges = {1: [0, 1, 2, 3], 2: [4, 5, 6, 7]}, {6: [0, 1, 2, 3], 7: [4, 5, 6, 7]}

    def super_block(s, _):
        xslot = lax.rem(s, 2)
        more = s + 1 < n_supers

        def before(k):
            if k == min(packs):
                when_do(more, frame_load(s + 1).wait)
            if k == min(merges):
                frames_cols_wait(1 - xslot, more)

        def beside(k):
            for u in packs.get(k, []):
                frames_pack(1 - xslot, u)
            for u in merges.get(k, []):
                frames_merge(1 - xslot, u)

        def after(k):
            if k == max(packs):
                for h in range(2):
                    when_do(jnp.logical_and(more, has_h[h]), frame_col(h, 1 - xslot).start)
                when_do(s + 2 < n_supers, frame_load(s + 2).start)
            if k == max(merges):
                for v in range(2):
                    when_do(jnp.logical_and(more, has_v[v]), frame_row(v, 1 - xslot).start)

        for bi in range(per_super):
            k = bi * ROW_STEPS
            t = s * COL_STEPS + k
            fresh = bi == 0
            ends = bi == per_super - 1
            before(k)
            if fresh:
                for g in range(n_groups):
                    col_take(g, xslot)
                    zr_rows(k, cuts[g], cuts[g + 1])
                beside(k)
                frames_rows_wait(xslot)
                spread(xslot, 0, 0, HR)
                spread(xslot, 0, HR + tile_h, far)
            else:
                zr_rows(k, 1, tile_h - 1)
                beside(k)
            after(k)
            row_take(bi % 2, fresh, xslot)
            zr_rows(k, -3, 1)
            zr_rows(k, tile_h - 1, tile_h + 3)
            n_rows_of(t, k, -2, tile_h + 2, True)
            spread(xslot, k + 1, 0, far)
            zr_rows(k + 1, -1, 5)
            zr_rows(k + 1, tile_h - 5, tile_h + 1)
            n_rows_of(t + 1, k + 1, 0, 4, not ends)
            n_rows_of(t + 1, k + 1, tile_h - 4, tile_h, not ends)
            before(k + 1)
            row_send((bi + 1) % 2, more if ends else True)
            zr_rows(k + 1, 5, tile_h - 5)
            beside(k + 1)
            after(k + 1)
            if ends:
                for g in range(n_groups):
                    a, b = max(PER * g, 4), min(PER * (g + 1), tile_h - 4)
                    n_rows_of(t + 1, k + 1, a, b, False)
                    col_send(g, 1 - xslot, more)
                spread(1 - xslot, 0, HR, HR + tile_h)
            else:
                n_rows_of(t + 1, k + 1, 4, tile_h - 4, True)
                spread(xslot, k + 2, 0, far)
        return 0
    lax.fori_loop(0, n_supers, super_block, 0)

    def last_row(i, _):
        hlast[i] = H[HR + i][:, :tile_w]
        return 0
    lax.fori_loop(0, tile_h, last_row, 0)


def solution(mesh):
    n_rows = mesh.shape['rows']
    n_cols = mesh.shape['cols']
    frame_spec = P(None, 'batch', 'rows', 'cols', None)
    state_spec = P('batch', 'rows', 'cols', None)

    def local_fn(frames, h_init, w_x, w_hzr, w_hn, gate_bias):
        steps, _, tile_h, tile_w, cin = frames.shape
        ch = h_init.shape[-1]
        total_rows = tile_h + 2 * HR
        groups = tile_h // PER
        vmem = pl.BlockSpec(memory_space=pltpu.VMEM)
        hbm = pl.BlockSpec(memory_space=pltpu.HBM)
        dma = pltpu.SemaphoreType.DMA
        corner = (ch * HR * HC // LANES, LANES)
        seq, last = pl.pallas_call(
            functools.partial(kernel, n_rows, n_cols),
            out_shape=(jax.ShapeDtypeStruct((steps, tile_h, ch, tile_w), BF),
                       jax.ShapeDtypeStruct((tile_h, ch, tile_w), F32)),
            in_specs=[hbm] * 6,
            out_specs=(vmem, vmem),
            scratch_shapes=[
                pltpu.VMEM((total_rows, ch, LANES), F32),
                pltpu.VMEM((total_rows * 3 * ch, LANES), BF),
                pltpu.VMEM((total_rows * 3 * ch, LANES), BF),
                pltpu.VMEM((2 * total_rows * 3 * cin, LANES), BF),
                pltpu.VMEM((total_rows, ch, LANES), F32),
                pltpu.VMEM((12 * ch + 12 * cin + 64, LANES), F32),
                pltpu.VMEM((2 * ch, 9 * ch + 9 * cin + 48), BF),
                pltpu.VMEM((2 * ch, 12 * ch + 12 * cin + 64), BF),
                pltpu.VMEM((tile_h, ch, tile_w), F32),
                pltpu.VMEM((9 * cin, 3 * ch), BF),
                pltpu.VMEM((9 * ch, 2 * ch), BF),
                pltpu.VMEM((9 * ch, ch), BF),
                pltpu.VMEM((1, 3 * ch), F32),
                pltpu.VMEM((COL_STEPS, tile_h, cin, tile_w), BF),
                pltpu.VMEM((2, COL_STEPS, total_rows, cin, LANES), BF),
                pltpu.VMEM((2, COL_STEPS, groups, cin, LANES), BF),
                pltpu.VMEM((2, 2, COL_STEPS, groups, cin, LANES), BF),
                pltpu.VMEM((2, groups, ch, LANES), F32),
                pltpu.VMEM((2, 2, groups, ch, LANES), F32),
                pltpu.VMEM((2, 2) + corner, F32),
                pltpu.VMEM((2, 2, 2) + corner, F32),
                pltpu.VMEM((2, HR, ch, LANES), F32),
                pltpu.VMEM((2, 2, HR, ch, LANES), F32),
                dma(()), dma((4,)), dma(()), dma((2,)), dma((2, 2)), dma((2,)), dma((2, 2)),
                dma((2, groups)), dma((2, 2, groups)), dma((2, 2)), dma((2, 2, 2)), dma((2,)), dma((2, 2)),
            ],
            compiler_params=pltpu.CompilerParams(collective_id=0, has_side_effects=True, vmem_limit_bytes=VMEM_MIB * 1024 * 1024),
        )(*[pltpu.with_memory_space_constraint(a, pltpu.HBM) for a in (
            frames[:, 0].transpose(0, 1, 3, 2), h_init[0].transpose(0, 2, 1), w_x.reshape(9 * cin, 3 * ch),
            w_hzr.reshape(9 * ch, 2 * ch), w_hn.reshape(9 * ch, ch), gate_bias[None])])
        return seq.transpose(0, 1, 3, 2)[:, None], last.transpose(0, 2, 1)[None]

    return jax.shard_map(local_fn, mesh=mesh, in_specs=(frame_spec, state_spec, P(), P(), P(), P()), out_specs=(frame_spec, state_spec), check_vma=False)
```

```python
import functools

import jax
import jax.numpy as jnp
from jax import lax
from jax.experimental import pallas as pl
from jax.experimental.pallas import tpu as pltpu
from jax.sharding import PartitionSpec as P

MESH = pl.DeviceIdType.MESH
LANES = 128
BF = jnp.bfloat16
F32 = jnp.float32

ROW_STEPS = 2
HR = 2 * ROW_STEPS
HC = 8
COL_STEPS = HC // 2
VMEM_MIB = 24
PER = LANES // HC


def store3(buf, base, size, val):
    buf[pl.ds(base, size), :] = pltpu.roll(val, 1, 1).astype(BF)
    buf[pl.ds(base + size, size), :] = val.astype(BF)
    buf[pl.ds(base + 2 * size, size), :] = pltpu.roll(val, LANES - 1, 1).astype(BF)


def spin(val, shift):
    shift = shift % LANES
    return pltpu.roll(val, shift, 1) if shift else val


def kernel(n_rows, n_cols, frames, h0, w_x_in, w_hzr_in, w_hn_in, bias_in, out, hlast,
           H, HB, RB, XB, Z, KM, WZR, WN, HI, w_x, w_hzr, w_hn, bias, FS, XF, FC, FR, CS, CR, DS, DR, RS, RR,
           hi_sem, w_sem, fs_sem, fc_send, fc_recv, fh_send, fh_recv,
           cs_send, cs_recv, dg_send, dg_recv, rr_send, rr_recv):
    steps, tile_h, ch, tile_w = out.shape
    cin = frames.shape[2]
    total_rows = tile_h + 2 * HR
    n_slots = tile_w // HC
    n_groups = tile_h // PER
    n_supers = steps // COL_STEPS
    per_super = COL_STEPS // ROW_STEPS
    row = lax.axis_index('rows')
    col = lax.axis_index('cols')
    has_v = (row > 0, row < n_rows - 1)
    has_h = (col > 0, col < n_cols - 1)
    diag = [(v, h, jnp.logical_and(has_v[v], has_h[h])) for v in range(2) for h in range(2)]

    def v_dev(v):
        return {'rows': row + 2 * v - 1}

    def h_dev(h):
        return {'cols': col + 2 * h - 1}

    def remote(src, dst, send, recv, dev):
        return pltpu.make_async_remote_copy(src, dst, send, recv, device_id=dev, device_id_type=MESH)

    def when_do(cond, *fns):
        @pl.when(cond)
        def _():
            for fn in fns:
                fn()

    lane = lax.broadcasted_iota(jnp.int32, (ch, LANES), 1)
    slot_of = lane // HC
    lane_x = lax.broadcasted_iota(jnp.int32, (cin, LANES), 1)
    slot_x = lane_x // HC
    middle = (tile_w + HC + LANES - HC) // 2
    ones = jnp.where(lax.broadcasted_iota(jnp.int32, (64, LANES), 0) < 3, 1.0, 0.0).astype(BF)
    ok = [jnp.where(c, 1, 0) for c in has_v + has_h]
    lane_ok = jnp.where(lane < tile_w, 1, jnp.where(lane < tile_w + HC, ok[3], jnp.where(lane >= LANES - HC, ok[2], 0)))
    lead = n_slots - 1

    def strip_masks(slots):
        return [jnp.logical_or(slots == q, slots == (lead + q) % PER) for q in range(PER)]

    def pack_rows(rows, slots, dtype, masks):
        acc = [jnp.zeros(rows[0].shape, dtype), jnp.zeros(rows[0].shape, dtype)]
        for q, val in enumerate(rows):
            acc[q % 2] = jnp.where(masks[q], spin(val, HC * q), acc[q % 2])
        even = slots % 2 == 0
        return jnp.where(even, acc[0], acc[1]), jnp.where(even, acc[1], acc[0])

    def halo_rows(from_left, from_right, slots):
        turned = spin(from_left, HC * (PER - 1 - n_slots - lead))
        even = slots % 2 == 0
        mixed = (jnp.where(even, from_right, turned), jnp.where(even, turned, from_right))
        return [spin(mixed[q % 2], HC * (n_slots - q)) for q in range(PER)]

    def frame_load(s):
        return pltpu.make_async_copy(frames.at[pl.ds(s * COL_STEPS, COL_STEPS)], FS, fs_sem)

    def frame_col(h, xslot):
        return remote(FC.at[h], FR.at[xslot, 1 - h], fc_send.at[h], fc_recv.at[xslot, 1 - h], h_dev(h))

    def frame_row(v, xslot):
        src = XF.at[xslot, :, pl.ds(HR + v * (tile_h - HR), HR)]
        dst = XF.at[xslot, :, pl.ds((1 - v) * (tile_h + HR), HR)]
        return remote(src, dst, fh_send.at[v], fh_recv.at[xslot, 1 - v], v_dev(v))

    def frames_pack(xslot, t):
        masks = strip_masks(slot_x)
        for g in range(n_groups):
            rows = []
            for q in range(PER):
                r = g * PER + q
                XF[xslot, t, HR + r, :, 0:tile_w] = FS[t, r]
                rows.append(XF[xslot, t, HR + r])
            FC[0, t, g], FC[1, t, g] = pack_rows(rows, slot_x, BF, masks)

    def frames_merge(xslot, t):
        own = lane_x < tile_w
        for g in range(n_groups):
            halos = halo_rows(FR[xslot, 0, t, g], FR[xslot, 1, t, g], slot_x)
            for q in range(PER):
                r = HR + g * PER + q
                XF[xslot, t, r] = jnp.where(own, XF[xslot, t, r], halos[q])

    def frames_cols_wait(xslot, cond):
        for h in range(2):
            when_do(jnp.logical_and(cond, has_h[h]), frame_col(h, xslot).wait_send, frame_col(1 - h, xslot).wait_recv)

    def frames_rows_wait(xslot):
        for v in range(2):
            when_do(has_v[v], frame_row(v, xslot).wait_send, frame_row(1 - v, xslot).wait_recv)

    def spread(xslot, k, first, last):
        for i in range(first, last):
            store3(XB, ((k % 2) * total_rows + i) * (3 * cin), cin, XF[xslot, k, i])

    def col_copy(h, g, slot):
        return remote(CS.at[h, g], CR.at[slot, 1 - h, g], cs_send.at[h, g], cs_recv.at[slot, 1 - h, g], h_dev(h))

    def diag_copy(v, h, slot):
        return remote(DS.at[v, h], DR.at[slot, 1 - v, 1 - h], dg_send.at[v, h], dg_recv.at[slot, 1 - v, 1 - h], {**v_dev(v), **h_dev(h)})

    def row_copy(v, slot):
        return remote(RS.at[v], RR.at[slot, 1 - v], rr_send.at[v], rr_recv.at[slot, 1 - v], v_dev(v))

    wide = HR * HC
    quarter = lax.broadcasted_iota(jnp.int32, (ch * wide // LANES, LANES), 1) // wide
    parts = LANES // wide
    part_ch = ch // parts

    def col_send(g, slot, cond):
        edges = pack_rows([H[HR + g * PER + q] for q in range(PER)], slot_of, F32, strip_masks(slot_of))
        for h in range(2):
            CS[h, g] = edges[h]
        for v in range(2):
            if g == (0 if v == 0 else n_groups - 1):
                for h in range(2):
                    first = (0 if v == 0 else PER - HR) + h * lead
                    small = jnp.zeros((part_ch, LANES), F32)
                    for c in range(parts):
                        small = jnp.where(quarter == c, spin(edges[h][c * part_ch:(c + 1) * part_ch], wide * c - HC * first), small)
                    DS[v, h] = small
        for h in range(2):
            when_do(jnp.logical_and(cond, has_h[h]), col_copy(h, g, slot).start)
        for v, h, both in diag:
            if g == (0 if v == 0 else n_groups - 1):
                when_do(jnp.logical_and(cond, both), diag_copy(v, h, slot).start)

    def col_take(g, slot):
        for h in range(2):
            when_do(has_h[h], col_copy(h, g, slot).wait_send, col_copy(1 - h, g, slot).wait_recv)
        halos = halo_rows(CR[slot, 0, g], CR[slot, 1, g], slot_of)
        own = lane < tile_w
        for q in range(PER):
            i = HR + g * PER + q
            val = jnp.where(own, H[i], halos[q])
            H[i] = val
            store3(HB, i * 3 * ch, ch, val)

    def row_send(slot, cond):
        RS[0] = H[HR:2 * HR]
        RS[1] = H[tile_h:tile_h + HR]
        for v in range(2):
            when_do(jnp.logical_and(cond, has_v[v]), row_copy(v, slot).start)

    def row_take(slot, fresh, cslot):
        for v in range(2):
            when_do(has_v[v], row_copy(v, slot).wait_send, row_copy(1 - v, slot).wait_recv)
        if fresh:
            for v, h, cond in diag:
                when_do(cond, diag_copy(v, h, cslot).wait_send, diag_copy(1 - v, 1 - h, cslot).wait_recv)
        for v in range(2):
            for i in range(HR):
                at = i + v * (tile_h + HR)
                val = RR[slot, v, i]
                if fresh:
                    sides = []
                    for h, to in ((0, LANES - HC), (1, tile_w)):
                        small = DR[cslot, v, h]
                        sides.append(jnp.concatenate([spin(small, to - wide * c - HC * i) for c in range(parts)], axis=0))
                    val = jnp.where(lane < tile_w, val, jnp.where(lane < middle, sides[1], sides[0]))
                H[at] = val
                store3(HB, at * 3 * ch, ch, val)

    def frame_rows(k, i, count):
        return XB[pl.ds(((k % 2) * total_rows + i) * (3 * cin), count * 3 * cin), :]

    def zr_rows(k, first, last):
        ones_zr = ones[:48]
        for r in range(first, last, 2):
            i = HR + r
            cols = []
            for d in range(2):
                hb = HB[pl.ds((i + d - 1) * (3 * ch), 9 * ch), :]
                cols.append(jnp.concatenate([hb, frame_rows(k, i + d - 1, 3), ones_zr], axis=0))
            acc = jnp.dot(WZR[...], jnp.concatenate(cols, axis=1), preferred_element_type=F32)
            gates = jnp.tanh(acc)
            for d in range(2):
                Z[i + d] = gates[:ch, d * LANES:(d + 1) * LANES]
                reset = 0.5 * gates[ch:, d * LANES:(d + 1) * LANES] + 0.5
                store3(RB, (i + d) * (3 * ch), ch, reset * H[i + d])

    def n_rows_of(t, k, first, last, keep):
        keep_in = lane_ok != 0
        for r in range(first, last, 4):
            i = HR + r
            cols = []
            for p in range(2):
                y = i + 2 * p - 1
                cols.append(jnp.concatenate([RB[pl.ds(y * (3 * ch), 12 * ch), :], frame_rows(k, y, 4), ones], axis=0))
            acc = jnp.dot(WN[...], jnp.concatenate(cols, axis=1), preferred_element_type=F32)
            cand = jnp.tanh(acc)
            for p in range(2):
                for dy in range(2):
                    at = i + 2 * p + dy
                    inside = HR <= at < HR + tile_h
                    cand_row = cand[dy * ch:(dy + 1) * ch, p * LANES:(p + 1) * LANES]
                    update = 0.5 * Z[at] + 0.5
                    new = cand_row + update * (H[at] - cand_row)
                    mask = keep_in if inside else lane_ok * (ok[0] if at < HR else ok[1]) != 0
                    new = jnp.where(mask, new, 0.0)
                    H[at] = new
                    new_bf = new.astype(BF)
                    if keep:
                        store3(HB, at * (3 * ch), ch, new)
                    if inside:
                        out[t, at - HR] = new_bf[:, :tile_w]

    def prepare_weights():
        def split3(val):
            top = float(jnp.finfo(BF).max)
            parts3 = []
            for _ in range(3):
                part = jnp.clip(val, -top, top).astype(BF).astype(F32)
                parts3.append(part)
                val = val - part
            return parts3

        def bias_rows(vals, count):
            at = lax.broadcasted_iota(jnp.int32, (count, LANES), 0)
            rows = jnp.zeros((count, LANES), F32)
            for n, part in enumerate(split3(vals)):
                rows = jnp.where(at == n, jnp.broadcast_to(part, (count, LANES)), rows)
            return rows

        def turn(dst):
            for c in range(dst.shape[1] // LANES):
                dst[:, c * LANES:(c + 1) * LANES] = KM[c * LANES:(c + 1) * LANES, :].T.astype(BF)

        taps, xtaps = 9 * ch, 9 * cin
        KM[0:taps] = 0.5 * w_hzr[...].astype(F32)
        KM[taps:taps + xtaps] = 0.5 * w_x[:, 0:2 * ch].astype(F32)
        KM[taps + xtaps:taps + xtaps + 48] = bias_rows(0.5 * bias[:, 0:2 * ch], 48)
        turn(WZR)

        def both(w, step):
            gap = jnp.zeros((step, ch), F32)
            return jnp.concatenate([jnp.concatenate([w, gap], axis=0), jnp.concatenate([gap, w], axis=0)], axis=1)
        KM[0:12 * ch] = both(w_hn[...].astype(F32), 3 * ch)
        KM[12 * ch:12 * ch + 12 * cin] = both(w_x[:, 2 * ch:3 * ch].astype(F32), 3 * cin)
        bias_n = bias[:, 2 * ch:3 * ch]
        KM[12 * ch + 12 * cin:12 * ch + 12 * cin + 64] = bias_rows(jnp.concatenate([bias_n, bias_n], axis=1), 64)
        turn(WN)

    frame_load(0).start()
    h_load = pltpu.make_async_copy(h0, HI, hi_sem)
    h_load.start()
    w_loads = [pltpu.make_async_copy(src, dst, w_sem.at[n]) for n, (src, dst) in enumerate(
        ((w_x_in, w_x), (w_hzr_in, w_hzr), (w_hn_in, w_hn), (bias_in, bias)))]
    for load in w_loads:
        load.start()
    for s in range(2):
        for side in range(2):
            CR[s, side] = jnp.zeros(CR.shape[2:], F32)
            DR[s, side] = jnp.zeros(DR.shape[2:], F32)
            RR[s, side] = jnp.zeros(RR.shape[2:], F32)
            FR[s, side] = jnp.zeros(FR.shape[2:], BF)
            for k in range(COL_STEPS):
                XF[s, k, pl.ds(side * (tile_h + HR), HR)] = jnp.zeros((HR, cin, LANES), BF)

    barrier = pltpu.get_barrier_semaphore()
    peers = [(has_v[v], v_dev(v)) for v in range(2)] + [(has_h[h], h_dev(h)) for h in range(2)]
    peers += [(cond, {**v_dev(v), **h_dev(h)}) for v, h, cond in diag]
    for cond, dev in peers:
        @pl.when(cond)
        def _(dev=dev):
            pl.semaphore_signal(barrier, inc=1, device_id=dev, device_id_type=MESH)
    h_load.wait()

    def init_row(i, _):
        H[i] = jnp.zeros((ch, LANES), F32)
        H[i, :, 0:tile_w] = HI[i - HR]
        return 0
    lax.fori_loop(HR, HR + tile_h, init_row, 0)
    frame_load(0).wait()
    for t in range(COL_STEPS):
        frames_pack(0, t)
    frame_load(1).start()
    pl.semaphore_wait(barrier, sum(jnp.where(cond, 1, 0) for cond, _ in peers))
    for h in range(2):
        when_do(has_h[h], frame_col(h, 0).start)
    row_send(0, True)
    for g in range(n_groups):
        col_send(g, 0, True)
    for load in w_loads:
        load.wait()
    prepare_weights()
    frames_cols_wait(0, True)
    for t in range(COL_STEPS):
        frames_merge(0, t)
    for v in range(2):
        when_do(has_v[v], frame_row(v, 0).start)
    spread(0, 0, HR, HR + tile_h)

    cuts = [PER * g - 1 if g else 1 for g in range(n_groups)] + [tile_h - 1]
    far = total_rows

    if COL_STEPS == 4:
        packs, merges = {0: [0, 1], 1: [2, 3]}, {3: [0, 1, 2, 3]}
    else:
        packs, merges = {1: [0, 1, 2, 3], 2: [4, 5, 6, 7]}, {6: [0, 1, 2, 3], 7: [4, 5, 6, 7]}

    def super_block(s, _):
        xslot = lax.rem(s, 2)
        more = s + 1 < n_supers

        def before(k):
            if k == min(packs):
                when_do(more, frame_load(s + 1).wait)
            if k == min(merges):
                frames_cols_wait(1 - xslot, more)

        def beside(k):
            for u in packs.get(k, []):
                frames_pack(1 - xslot, u)
            for u in merges.get(k, []):
                frames_merge(1 - xslot, u)

        def after(k):
            if k == max(packs):
                for h in range(2):
                    when_do(jnp.logical_and(more, has_h[h]), frame_col(h, 1 - xslot).start)
                when_do(s + 2 < n_supers, frame_load(s + 2).start)
            if k == max(merges):
                for v in range(2):
                    when_do(jnp.logical_and(more, has_v[v]), frame_row(v, 1 - xslot).start)

        for bi in range(per_super):
            k = bi * ROW_STEPS
            t = s * COL_STEPS + k
            fresh = bi == 0
            ends = bi == per_super - 1
            before(k)
            if fresh:
                for g in range(n_groups):
                    col_take(g, xslot)
                    zr_rows(k, cuts[g], cuts[g + 1])
                beside(k)
                frames_rows_wait(xslot)
                spread(xslot, 0, 0, HR)
                spread(xslot, 0, HR + tile_h, far)
            else:
                zr_rows(k, 1, tile_h - 1)
                beside(k)
            after(k)
            if not fresh:
                n_rows_of(t, k, 2, tile_h - 2, True)
            row_take(bi % 2, fresh, xslot)
            zr_rows(k, -3, 1)
            zr_rows(k, tile_h - 1, tile_h + 3)
            if fresh:
                n_rows_of(t, k, -2, tile_h + 2, True)
            else:
                n_rows_of(t, k, -2, 2, True)
                n_rows_of(t, k, tile_h - 2, tile_h + 2, True)
            spread(xslot, k + 1, 0, far)
            zr_rows(k + 1, -1, 5)
            zr_rows(k + 1, tile_h - 5, tile_h + 1)
            n_rows_of(t + 1, k + 1, 0, 4, not ends)
            n_rows_of(t + 1, k + 1, tile_h - 4, tile_h, not ends)
            before(k + 1)
            row_send((bi + 1) % 2, more if ends else True)
            late = PER * (n_groups - 1) + 1 if ends else tile_h - 5
            zr_rows(k + 1, 5, late)
            beside(k + 1)
            after(k + 1)
            if ends:
                for g in range(n_groups):
                    a, b = max(PER * g, 4), min(PER * (g + 1), tile_h - 4)
                    if g == 1:
                        zr_rows(k + 1, late, tile_h - 5)
                    n_rows_of(t + 1, k + 1, a, b, False)
                    col_send(g, 1 - xslot, more)
                spread(1 - xslot, 0, HR, HR + tile_h)
            else:
                n_rows_of(t + 1, k + 1, 4, tile_h - 4, True)
                spread(xslot, k + 2, 0, far)
        return 0
    lax.fori_loop(0, n_supers, super_block, 0)

    def last_row(i, _):
        hlast[i] = H[HR + i][:, :tile_w]
        return 0
    lax.fori_loop(0, tile_h, last_row, 0)


def solution(mesh):
    n_rows = mesh.shape['rows']
    n_cols = mesh.shape['cols']
    frame_spec = P(None, 'batch', 'rows', 'cols', None)
    state_spec = P('batch', 'rows', 'cols', None)

    def local_fn(frames, h_init, w_x, w_hzr, w_hn, gate_bias):
        steps, _, tile_h, tile_w, cin = frames.shape
        ch = h_init.shape[-1]
        total_rows = tile_h + 2 * HR
        groups = tile_h // PER
        vmem = pl.BlockSpec(memory_space=pltpu.VMEM)
        hbm = pl.BlockSpec(memory_space=pltpu.HBM)
        dma = pltpu.SemaphoreType.DMA
        corner = (ch * HR * HC // LANES, LANES)
        seq, last = pl.pallas_call(
            functools.partial(kernel, n_rows, n_cols),
            out_shape=(jax.ShapeDtypeStruct((steps, tile_h, ch, tile_w), BF),
                       jax.ShapeDtypeStruct((tile_h, ch, tile_w), F32)),
            in_specs=[hbm] * 6,
            out_specs=(vmem, vmem),
            scratch_shapes=[
                pltpu.VMEM((total_rows, ch, LANES), F32),
                pltpu.VMEM((total_rows * 3 * ch, LANES), BF),
                pltpu.VMEM((total_rows * 3 * ch, LANES), BF),
                pltpu.VMEM((2 * total_rows * 3 * cin, LANES), BF),
                pltpu.VMEM((total_rows, ch, LANES), F32),
                pltpu.VMEM((12 * ch + 12 * cin + 64, LANES), F32),
                pltpu.VMEM((2 * ch, 9 * ch + 9 * cin + 48), BF),
                pltpu.VMEM((2 * ch, 12 * ch + 12 * cin + 64), BF),
                pltpu.VMEM((tile_h, ch, tile_w), F32),
                pltpu.VMEM((9 * cin, 3 * ch), BF),
                pltpu.VMEM((9 * ch, 2 * ch), BF),
                pltpu.VMEM((9 * ch, ch), BF),
                pltpu.VMEM((1, 3 * ch), F32),
                pltpu.VMEM((COL_STEPS, tile_h, cin, tile_w), BF),
                pltpu.VMEM((2, COL_STEPS, total_rows, cin, LANES), BF),
                pltpu.VMEM((2, COL_STEPS, groups, cin, LANES), BF),
                pltpu.VMEM((2, 2, COL_STEPS, groups, cin, LANES), BF),
                pltpu.VMEM((2, groups, ch, LANES), F32),
                pltpu.VMEM((2, 2, groups, ch, LANES), F32),
                pltpu.VMEM((2, 2) + corner, F32),
                pltpu.VMEM((2, 2, 2) + corner, F32),
                pltpu.VMEM((2, HR, ch, LANES), F32),
                pltpu.VMEM((2, 2, HR, ch, LANES), F32),
                dma(()), dma((4,)), dma(()), dma((2,)), dma((2, 2)), dma((2,)), dma((2, 2)),
                dma((2, groups)), dma((2, 2, groups)), dma((2, 2)), dma((2, 2, 2)), dma((2,)), dma((2, 2)),
            ],
            compiler_params=pltpu.CompilerParams(collective_id=0, has_side_effects=True, vmem_limit_bytes=VMEM_MIB * 1024 * 1024),
        )(*[pltpu.with_memory_space_constraint(a, pltpu.HBM) for a in (
            frames[:, 0].transpose(0, 1, 3, 2), h_init[0].transpose(0, 2, 1), w_x.reshape(9 * cin, 3 * ch),
            w_hzr.reshape(9 * ch, 2 * ch), w_hn.reshape(9 * ch, ch), gate_bias[None])])
        return seq.transpose(0, 1, 3, 2)[:, None], last.transpose(0, 2, 1)[None]

    return jax.shard_map(local_fn, mesh=mesh, in_specs=(frame_spec, state_spec, P(), P(), P(), P()), out_specs=(frame_spec, state_spec), check_vma=False)
```

```python
import functools

import jax
import jax.numpy as jnp
from jax import lax
from jax.experimental import pallas as pl
from jax.experimental.pallas import tpu as pltpu
from jax.sharding import PartitionSpec as P

MESH = pl.DeviceIdType.MESH
LANES = 128
BF = jnp.bfloat16
F32 = jnp.float32

ROW_STEPS = 2
HR = 2 * ROW_STEPS
HC = 8
COL_STEPS = HC // 2
VMEM_MIB = 24
PER = LANES // HC


def store3(buf, base, size, val):
    buf[pl.ds(base, size), :] = pltpu.roll(val, 1, 1).astype(BF)
    buf[pl.ds(base + size, size), :] = val.astype(BF)
    buf[pl.ds(base + 2 * size, size), :] = pltpu.roll(val, LANES - 1, 1).astype(BF)


def spin(val, shift):
    shift = shift % LANES
    return pltpu.roll(val, shift, 1) if shift else val


def kernel(n_rows, n_cols, frames, h0, w_x_in, w_hzr_in, w_hn_in, bias_in, out, hlast,
           H, HB, RB, XB, Z, KM, WZR, WN, HI, w_x, w_hzr, w_hn, bias, FS, XF, FC, FR, CS, CR, DS, DR, RS, RR,
           hi_sem, w_sem, fs_sem, fc_send, fc_recv, fh_send, fh_recv,
           cs_send, cs_recv, dg_send, dg_recv, rr_send, rr_recv):
    steps, tile_h, ch, tile_w = out.shape
    cin = frames.shape[2]
    total_rows = tile_h + 2 * HR
    n_slots = tile_w // HC
    n_groups = tile_h // PER
    n_supers = steps // COL_STEPS
    per_super = COL_STEPS // ROW_STEPS
    row = lax.axis_index('rows')
    col = lax.axis_index('cols')
    has_v = (row > 0, row < n_rows - 1)
    has_h = (col > 0, col < n_cols - 1)
    diag = [(v, h, jnp.logical_and(has_v[v], has_h[h])) for v in range(2) for h in range(2)]

    def v_dev(v):
        return {'rows': row + 2 * v - 1}

    def h_dev(h):
        return {'cols': col + 2 * h - 1}

    def remote(src, dst, send, recv, dev):
        return pltpu.make_async_remote_copy(src, dst, send, recv, device_id=dev, device_id_type=MESH)

    def when_do(cond, *fns):
        @pl.when(cond)
        def _():
            for fn in fns:
                fn()

    lane = lax.broadcasted_iota(jnp.int32, (ch, LANES), 1)
    slot_of = lane // HC
    lane_x = lax.broadcasted_iota(jnp.int32, (cin, LANES), 1)
    slot_x = lane_x // HC
    middle = (tile_w + HC + LANES - HC) // 2
    ones = jnp.where(lax.broadcasted_iota(jnp.int32, (64, LANES), 0) < 3, 1.0, 0.0).astype(BF)
    ok = [jnp.where(c, 1, 0) for c in has_v + has_h]
    lane_ok = jnp.where(lane < tile_w, 1, jnp.where(lane < tile_w + HC, ok[3], jnp.where(lane >= LANES - HC, ok[2], 0)))
    lead = n_slots - 1

    def strip_masks(slots):
        return [jnp.logical_or(slots == q, slots == (lead + q) % PER) for q in range(PER)]

    def pack_rows(rows, slots, dtype, masks):
        acc = [jnp.zeros(rows[0].shape, dtype), jnp.zeros(rows[0].shape, dtype)]
        for q, val in enumerate(rows):
            acc[q % 2] = jnp.where(masks[q], spin(val, HC * q), acc[q % 2])
        even = slots % 2 == 0
        return jnp.where(even, acc[0], acc[1]), jnp.where(even, acc[1], acc[0])

    def halo_rows(from_left, from_right, slots):
        turned = spin(from_left, HC * (PER - 1 - n_slots - lead))
        even = slots % 2 == 0
        mixed = (jnp.where(even, from_right, turned), jnp.where(even, turned, from_right))
        return [spin(mixed[q % 2], HC * (n_slots - q)) for q in range(PER)]

    def frame_load(s):
        return pltpu.make_async_copy(frames.at[pl.ds(s * COL_STEPS, COL_STEPS)], FS, fs_sem)

    def frame_col(h, xslot):
        return remote(FC.at[h], FR.at[xslot, 1 - h], fc_send.at[h], fc_recv.at[xslot, 1 - h], h_dev(h))

    def frame_row(v, xslot):
        src = XF.at[xslot, :, pl.ds(HR + v * (tile_h - HR), HR)]
        dst = XF.at[xslot, :, pl.ds((1 - v) * (tile_h + HR), HR)]
        return remote(src, dst, fh_send.at[v], fh_recv.at[xslot, 1 - v], v_dev(v))

    def frames_pack(xslot, t):
        masks = strip_masks(slot_x)
        for g in range(n_groups):
            rows = []
            for q in range(PER):
                r = g * PER + q
                XF[xslot, t, HR + r, :, 0:tile_w] = FS[t, r]
                rows.append(XF[xslot, t, HR + r])
            FC[0, t, g], FC[1, t, g] = pack_rows(rows, slot_x, BF, masks)

    def frames_merge(xslot, t):
        own = lane_x < tile_w
        for g in range(n_groups):
            halos = halo_rows(FR[xslot, 0, t, g], FR[xslot, 1, t, g], slot_x)
            for q in range(PER):
                r = HR + g * PER + q
                XF[xslot, t, r] = jnp.where(own, XF[xslot, t, r], halos[q])

    def frames_cols_wait(xslot, cond):
        for h in range(2):
            when_do(jnp.logical_and(cond, has_h[h]), frame_col(h, xslot).wait_send, frame_col(1 - h, xslot).wait_recv)

    def frames_rows_wait(xslot):
        for v in range(2):
            when_do(has_v[v], frame_row(v, xslot).wait_send, frame_row(1 - v, xslot).wait_recv)

    def spread(xslot, k, first, last):
        for i in range(first, last):
            store3(XB, ((k % 2) * total_rows + i) * (3 * cin), cin, XF[xslot, k, i])

    def col_copy(h, g, slot):
        return remote(CS.at[h, g], CR.at[slot, 1 - h, g], cs_send.at[h, g], cs_recv.at[slot, 1 - h, g], h_dev(h))

    def diag_copy(v, h, slot):
        return remote(DS.at[v, h], DR.at[slot, 1 - v, 1 - h], dg_send.at[v, h], dg_recv.at[slot, 1 - v, 1 - h], {**v_dev(v), **h_dev(h)})

    def row_copy(v, slot):
        return remote(RS.at[v], RR.at[slot, 1 - v], rr_send.at[v], rr_recv.at[slot, 1 - v], v_dev(v))

    wide = HR * HC
    quarter = lax.broadcasted_iota(jnp.int32, (ch * wide // LANES, LANES), 1) // wide
    parts = LANES // wide
    part_ch = ch // parts

    def col_send(g, slot, cond):
        edges = pack_rows([H[HR + g * PER + q] for q in range(PER)], slot_of, F32, strip_masks(slot_of))
        for h in range(2):
            CS[h, g] = edges[h]
        for h in range(2):
            when_do(jnp.logical_and(cond, has_h[h]), col_copy(h, g, slot).start)
        for v in range(2):
            if g == (0 if v == 0 else n_groups - 1):
                for h in range(2):
                    first = (0 if v == 0 else PER - HR) + h * lead
                    small = jnp.zeros((part_ch, LANES), F32)
                    for c in range(parts):
                        small = jnp.where(quarter == c, spin(edges[h][c * part_ch:(c + 1) * part_ch], wide * c - HC * first), small)
                    DS[v, h] = small
        for v, h, both in diag:
            if g == (0 if v == 0 else n_groups - 1):
                when_do(jnp.logical_and(cond, both), diag_copy(v, h, slot).start)

    def col_take(g, slot):
        for h in range(2):
            when_do(has_h[h], col_copy(h, g, slot).wait_send, col_copy(1 - h, g, slot).wait_recv)
        halos = halo_rows(CR[slot, 0, g], CR[slot, 1, g], slot_of)
        own = lane < tile_w
        for q in range(PER):
            i = HR + g * PER + q
            val = jnp.where(own, H[i], halos[q])
            H[i] = val
            store3(HB, i * 3 * ch, ch, val)

    def row_send(slot, cond):
        RS[0] = H[HR:2 * HR]
        RS[1] = H[tile_h:tile_h + HR]
        for v in range(2):
            when_do(jnp.logical_and(cond, has_v[v]), row_copy(v, slot).start)

    def row_take(slot, fresh, cslot):
        for v in range(2):
            when_do(has_v[v], row_copy(v, slot).wait_send, row_copy(1 - v, slot).wait_recv)
        if fresh:
            for v, h, cond in diag:
                when_do(cond, diag_copy(v, h, cslot).wait_send, diag_copy(1 - v, 1 - h, cslot).wait_recv)
        for v in range(2):
            for i in range(HR):
                at = i + v * (tile_h + HR)
                val = RR[slot, v, i]
                if fresh:
                    sides = []
                    for h, to in ((0, LANES - HC), (1, tile_w)):
                        small = DR[cslot, v, h]
                        sides.append(jnp.concatenate([spin(small, to - wide * c - HC * i) for c in range(parts)], axis=0))
                    val = jnp.where(lane < tile_w, val, jnp.where(lane < middle, sides[1], sides[0]))
                H[at] = val
                store3(HB, at * 3 * ch, ch, val)

    def frame_rows(k, i, count):
        return XB[pl.ds(((k % 2) * total_rows + i) * (3 * cin), count * 3 * cin), :]

    def zr_rows(k, first, last):
        ones_zr = ones[:48]
        for r in range(first, last, 2):
            i = HR + r
            cols = []
            for d in range(2):
                hb = HB[pl.ds((i + d - 1) * (3 * ch), 9 * ch), :]
                cols.append(jnp.concatenate([hb, frame_rows(k, i + d - 1, 3), ones_zr], axis=0))
            acc = jnp.dot(WZR[...], jnp.concatenate(cols, axis=1), preferred_element_type=F32)
            gates = jnp.tanh(acc)
            for d in range(2):
                Z[i + d] = gates[:ch, d * LANES:(d + 1) * LANES]
                reset = 0.5 * gates[ch:, d * LANES:(d + 1) * LANES] + 0.5
                store3(RB, (i + d) * (3 * ch), ch, reset * H[i + d])

    def n_rows_of(t, k, first, last, keep):
        keep_in = lane_ok != 0
        for r in range(first, last, 4):
            i = HR + r
            cols = []
            for p in range(2):
                y = i + 2 * p - 1
                cols.append(jnp.concatenate([RB[pl.ds(y * (3 * ch), 12 * ch), :], frame_rows(k, y, 4), ones], axis=0))
            acc = jnp.dot(WN[...], jnp.concatenate(cols, axis=1), preferred_element_type=F32)
            cand = jnp.tanh(acc)
            for p in range(2):
                for dy in range(2):
                    at = i + 2 * p + dy
                    inside = HR <= at < HR + tile_h
                    cand_row = cand[dy * ch:(dy + 1) * ch, p * LANES:(p + 1) * LANES]
                    update = 0.5 * Z[at] + 0.5
                    new = cand_row + update * (H[at] - cand_row)
                    mask = keep_in if inside else lane_ok * (ok[0] if at < HR else ok[1]) != 0
                    new = jnp.where(mask, new, 0.0)
                    H[at] = new
                    new_bf = new.astype(BF)
                    if keep:
                        store3(HB, at * (3 * ch), ch, new)
                    if inside:
                        out[t, at - HR] = new_bf[:, :tile_w]

    def prepare_weights():
        def split3(val):
            top = float(jnp.finfo(BF).max)
            parts3 = []
            for _ in range(3):
                part = jnp.clip(val, -top, top).astype(BF).astype(F32)
                parts3.append(part)
                val = val - part
            return parts3

        def bias_rows(vals, count):
            at = lax.broadcasted_iota(jnp.int32, (count, LANES), 0)
            rows = jnp.zeros((count, LANES), F32)
            for n, part in enumerate(split3(vals)):
                rows = jnp.where(at == n, jnp.broadcast_to(part, (count, LANES)), rows)
            return rows

        def turn(dst):
            for c in range(dst.shape[1] // LANES):
                dst[:, c * LANES:(c + 1) * LANES] = KM[c * LANES:(c + 1) * LANES, :].T.astype(BF)

        taps, xtaps = 9 * ch, 9 * cin
        KM[0:taps] = 0.5 * w_hzr[...].astype(F32)
        KM[taps:taps + xtaps] = 0.5 * w_x[:, 0:2 * ch].astype(F32)
        KM[taps + xtaps:taps + xtaps + 48] = bias_rows(0.5 * bias[:, 0:2 * ch], 48)
        turn(WZR)

        def both(w, step):
            gap = jnp.zeros((step, ch), F32)
            return jnp.concatenate([jnp.concatenate([w, gap], axis=0), jnp.concatenate([gap, w], axis=0)], axis=1)
        KM[0:12 * ch] = both(w_hn[...].astype(F32), 3 * ch)
        KM[12 * ch:12 * ch + 12 * cin] = both(w_x[:, 2 * ch:3 * ch].astype(F32), 3 * cin)
        bias_n = bias[:, 2 * ch:3 * ch]
        KM[12 * ch + 12 * cin:12 * ch + 12 * cin + 64] = bias_rows(jnp.concatenate([bias_n, bias_n], axis=1), 64)
        turn(WN)

    frame_load(0).start()
    h_load = pltpu.make_async_copy(h0, HI, hi_sem)
    h_load.start()
    w_loads = [pltpu.make_async_copy(src, dst, w_sem.at[n]) for n, (src, dst) in enumerate(
        ((w_x_in, w_x), (w_hzr_in, w_hzr), (w_hn_in, w_hn), (bias_in, bias)))]
    for load in w_loads:
        load.start()
    for s in range(2):
        for side in range(2):
            CR[s, side] = jnp.zeros(CR.shape[2:], F32)
            DR[s, side] = jnp.zeros(DR.shape[2:], F32)
            RR[s, side] = jnp.zeros(RR.shape[2:], F32)
            FR[s, side] = jnp.zeros(FR.shape[2:], BF)
            for k in range(COL_STEPS):
                XF[s, k, pl.ds(side * (tile_h + HR), HR)] = jnp.zeros((HR, cin, LANES), BF)

    barrier = pltpu.get_barrier_semaphore()
    peers = [(has_v[v], v_dev(v)) for v in range(2)] + [(has_h[h], h_dev(h)) for h in range(2)]
    peers += [(cond, {**v_dev(v), **h_dev(h)}) for v, h, cond in diag]
    for cond, dev in peers:
        @pl.when(cond)
        def _(dev=dev):
            pl.semaphore_signal(barrier, inc=1, device_id=dev, device_id_type=MESH)
    h_load.wait()

    def init_row(i, _):
        H[i] = jnp.zeros((ch, LANES), F32)
        H[i, :, 0:tile_w] = HI[i - HR]
        return 0
    lax.fori_loop(HR, HR + tile_h, init_row, 0)
    frame_load(0).wait()
    for t in range(COL_STEPS):
        frames_pack(0, t)
    frame_load(1).start()
    pl.semaphore_wait(barrier, sum(jnp.where(cond, 1, 0) for cond, _ in peers))
    for h in range(2):
        when_do(has_h[h], frame_col(h, 0).start)
    row_send(0, True)
    for g in range(n_groups):
        col_send(g, 0, True)
    for load in w_loads:
        load.wait()
    prepare_weights()
    frames_cols_wait(0, True)
    for t in range(COL_STEPS):
        frames_merge(0, t)
    for v in range(2):
        when_do(has_v[v], frame_row(v, 0).start)
    spread(0, 0, HR, HR + tile_h)

    cuts = [PER * g - 1 if g else 1 for g in range(n_groups)] + [tile_h - 1]
    far = total_rows

    if COL_STEPS == 4:
        packs, merges = {0: [0, 1], 1: [2, 3]}, {3: [0, 1, 2, 3]}
    else:
        packs, merges = {1: [0, 1, 2, 3], 2: [4, 5, 6, 7]}, {6: [0, 1, 2, 3], 7: [4, 5, 6, 7]}

    def super_block(s, _):
        xslot = lax.rem(s, 2)
        more = s + 1 < n_supers

        def before(k):
            if k == min(packs):
                when_do(more, frame_load(s + 1).wait)
            if k == min(merges):
                frames_cols_wait(1 - xslot, more)

        def beside(k):
            for u in packs.get(k, []):
                frames_pack(1 - xslot, u)
            for u in merges.get(k, []):
                frames_merge(1 - xslot, u)

        def after(k):
            if k == max(packs):
                for h in range(2):
                    when_do(jnp.logical_and(more, has_h[h]), frame_col(h, 1 - xslot).start)
                when_do(s + 2 < n_supers, frame_load(s + 2).start)
            if k == max(merges):
                for v in range(2):
                    when_do(jnp.logical_and(more, has_v[v]), frame_row(v, 1 - xslot).start)

        for bi in range(per_super):
            k = bi * ROW_STEPS
            t = s * COL_STEPS + k
            fresh = bi == 0
            ends = bi == per_super - 1
            before(k)
            if fresh:
                for g in range(n_groups):
                    col_take(g, xslot)
                    zr_rows(k, cuts[g], cuts[g + 1])
                beside(k)
                frames_rows_wait(xslot)
                spread(xslot, 0, 0, HR)
                spread(xslot, 0, HR + tile_h, far)
            else:
                zr_rows(k, 1, tile_h - 1)
                beside(k)
            after(k)
            if not fresh:
                n_rows_of(t, k, 2, tile_h - 2, True)
            row_take(bi % 2, fresh, xslot)
            zr_rows(k, -3, 1)
            zr_rows(k, tile_h - 1, tile_h + 3)
            if fresh:
                n_rows_of(t, k, -2, tile_h + 2, True)
            else:
                n_rows_of(t, k, -2, 2, True)
                n_rows_of(t, k, tile_h - 2, tile_h + 2, True)
            spread(xslot, k + 1, 0, far)
            zr_rows(k + 1, -1, 5)
            zr_rows(k + 1, tile_h - 5, tile_h + 1)
            n_rows_of(t + 1, k + 1, 0, 4, not ends)
            n_rows_of(t + 1, k + 1, tile_h - 4, tile_h, not ends)
            before(k + 1)
            row_send((bi + 1) % 2, more if ends else True)
            late = PER * (n_groups - 1) + 1 if ends else tile_h - 5
            zr_rows(k + 1, 5, late)
            beside(k + 1)
            after(k + 1)
            if ends:
                for g in range(n_groups):
                    a, b = max(PER * g, 4), min(PER * (g + 1), tile_h - 4)
                    if g == 1:
                        zr_rows(k + 1, late, tile_h - 5)
                    n_rows_of(t + 1, k + 1, a, b, False)
                    col_send(g, 1 - xslot, more)
                spread(1 - xslot, 0, HR, HR + tile_h)
            else:
                n_rows_of(t + 1, k + 1, 4, tile_h - 4, True)
                spread(xslot, k + 2, 0, far)
        return 0
    lax.fori_loop(0, n_supers, super_block, 0)

    def last_row(i, _):
        hlast[i] = H[HR + i][:, :tile_w]
        return 0
    lax.fori_loop(0, tile_h, last_row, 0)


def solution(mesh):
    n_rows = mesh.shape['rows']
    n_cols = mesh.shape['cols']
    frame_spec = P(None, 'batch', 'rows', 'cols', None)
    state_spec = P('batch', 'rows', 'cols', None)

    def local_fn(frames, h_init, w_x, w_hzr, w_hn, gate_bias):
        steps, _, tile_h, tile_w, cin = frames.shape
        ch = h_init.shape[-1]
        total_rows = tile_h + 2 * HR
        groups = tile_h // PER
        vmem = pl.BlockSpec(memory_space=pltpu.VMEM)
        hbm = pl.BlockSpec(memory_space=pltpu.HBM)
        dma = pltpu.SemaphoreType.DMA
        corner = (ch * HR * HC // LANES, LANES)
        seq, last = pl.pallas_call(
            functools.partial(kernel, n_rows, n_cols),
            out_shape=(jax.ShapeDtypeStruct((steps, tile_h, ch, tile_w), BF),
                       jax.ShapeDtypeStruct((tile_h, ch, tile_w), F32)),
            in_specs=[hbm] * 6,
            out_specs=(vmem, vmem),
            scratch_shapes=[
                pltpu.VMEM((total_rows, ch, LANES), F32),
                pltpu.VMEM((total_rows * 3 * ch, LANES), BF),
                pltpu.VMEM((total_rows * 3 * ch, LANES), BF),
                pltpu.VMEM((2 * total_rows * 3 * cin, LANES), BF),
                pltpu.VMEM((total_rows, ch, LANES), F32),
                pltpu.VMEM((12 * ch + 12 * cin + 64, LANES), F32),
                pltpu.VMEM((2 * ch, 9 * ch + 9 * cin + 48), BF),
                pltpu.VMEM((2 * ch, 12 * ch + 12 * cin + 64), BF),
                pltpu.VMEM((tile_h, ch, tile_w), F32),
                pltpu.VMEM((9 * cin, 3 * ch), BF),
                pltpu.VMEM((9 * ch, 2 * ch), BF),
                pltpu.VMEM((9 * ch, ch), BF),
                pltpu.VMEM((1, 3 * ch), F32),
                pltpu.VMEM((COL_STEPS, tile_h, cin, tile_w), BF),
                pltpu.VMEM((2, COL_STEPS, total_rows, cin, LANES), BF),
                pltpu.VMEM((2, COL_STEPS, groups, cin, LANES), BF),
                pltpu.VMEM((2, 2, COL_STEPS, groups, cin, LANES), BF),
                pltpu.VMEM((2, groups, ch, LANES), F32),
                pltpu.VMEM((2, 2, groups, ch, LANES), F32),
                pltpu.VMEM((2, 2) + corner, F32),
                pltpu.VMEM((2, 2, 2) + corner, F32),
                pltpu.VMEM((2, HR, ch, LANES), F32),
                pltpu.VMEM((2, 2, HR, ch, LANES), F32),
                dma(()), dma((4,)), dma(()), dma((2,)), dma((2, 2)), dma((2,)), dma((2, 2)),
                dma((2, groups)), dma((2, 2, groups)), dma((2, 2)), dma((2, 2, 2)), dma((2,)), dma((2, 2)),
            ],
            compiler_params=pltpu.CompilerParams(collective_id=0, has_side_effects=True, vmem_limit_bytes=VMEM_MIB * 1024 * 1024),
        )(*[pltpu.with_memory_space_constraint(a, pltpu.HBM) for a in (
            frames[:, 0].transpose(0, 1, 3, 2), h_init[0].transpose(0, 2, 1), w_x.reshape(9 * cin, 3 * ch),
            w_hzr.reshape(9 * ch, 2 * ch), w_hn.reshape(9 * ch, ch), gate_bias[None])])
        return seq.transpose(0, 1, 3, 2)[:, None], last.transpose(0, 2, 1)[None]

    return jax.shard_map(local_fn, mesh=mesh, in_specs=(frame_spec, state_spec, P(), P(), P(), P()), out_specs=(frame_spec, state_spec), check_vma=False)
```
